128 devices in a mesh: grp: 8 (over y, x_lo), slab: 16 (over z, x_hi, core).
Axes of the slice: x: 4 (x_hi: 2, x_lo: 2; x = x_hi * 2 + x_lo), y: 4, z: 4, core: 2. Of those that a mesh axis runs over, the one named last changes fastest.
Arguments:
- forcing: float32 [8, 3, 128, 128, 128], P('grp', None, 'slab'), may hold values from -18 to 18
- stiffness: float32 [8, 3, 128, 128, 128], P('grp', None, 'slab'), may hold values from 0.25 to 4
- anisotropy: float32 [8, 3, 3], P('grp'), may hold values from 0.3 to 3
- coupling: float32 [8, 3, 3], P('grp'), may hold values from -0.3 to 2, as said below
- levels: int32 [8, 2], replicated, may hold values from 0 to 2
- neighbours: int32 [8, 3], replicated, may hold values from -1 to 7, as said below
Outputs:
- mixed: float32 [8, 3, 128, 128, 128], P('grp', None, 'slab')
The draws below stay inside these ranges and needn't reach their ends.
Inputs may be any that keep to these rules, and one draw needn't show every extreme that they name: neighbours[g, 0], [g, 1], [g, 2] name a pair whose levels are those of pair g less (1, 0), (0, 1), (1, 1), or are -1 where no pair has those levels. `coupling`: symmetric; diagonal entries 0.8 to 2, off-diagonal entries at most 0.3 in magnitude.
All inputs are finite; a program needn't handle non-finite values.
Results may differ from the reference program's by a relative error of at most 0.0003.
Values sent between devices are 32-bit elements; how exact they have to be, the bound alone decides.
A program may use at most 64 MiB of HBM per device.

```python
import math
import jax
import jax.numpy as jnp
from jax import lax

ZD = 8
XMAX = 128
Y = 128
ITERS = 2
PAIRS = 8
ZMAX = 128
N_SLAB = 16


def index_table(key):
    base_key = jax.random.fold_in(key, 5)
    level_key, top_key, order_key, score_key = jax.random.split(base_key, 4)
    loose = jax.random.randint(level_key, (PAIRS, 2), 0, 3, dtype=jnp.int32)
    blocks = PAIRS // 4 + 1
    tops = jax.random.randint(top_key, (blocks, 2), 1, 3, dtype=jnp.int32)
    block_rows = jnp.arange(blocks, dtype=jnp.int32)[:, None]
    tops = jnp.where(block_rows == 0, 2, tops).astype(jnp.int32)
    member = jnp.arange(PAIRS, dtype=jnp.int32)
    block_of = member // 4
    role = member % 4
    lowering = jnp.array([[0, 0], [1, 0], [0, 1], [1, 1]], dtype=jnp.int32)
    grouped = jnp.take(tops, block_of, axis=0) - jnp.take(lowering, role, axis=0)
    in_block = (block_of < PAIRS // 4)[:, None]
    ordered = jnp.where(in_block, grouped, loose).astype(jnp.int32)
    ordered = jnp.where((member == PAIRS - 1)[:, None], 0, ordered).astype(jnp.int32)
    order = jax.random.permutation(order_key, PAIRS).astype(jnp.int32)
    levels = jnp.take(ordered, order, axis=0).astype(jnp.int32)
    offsets = jnp.array([[1, 0], [0, 1], [1, 1]], dtype=jnp.int32)
    wanted = levels[:, None, :] - offsets[None]
    matching = jnp.all(levels[None, None, :, :] == wanted[:, :, None, :], axis=-1)
    scores = jax.random.randint(score_key, (PAIRS, 3, PAIRS), 0, 65536, dtype=jnp.int32) * PAIRS
    scores = scores + jnp.arange(PAIRS, dtype=jnp.int32)[None, None, :]
    scores = jnp.where(matching, scores, -1)
    chosen = lax.top_k(scores, 1)[1][..., 0].astype(jnp.int32)
    linked = jnp.where(jnp.any(matching, axis=-1), chosen, -1).astype(jnp.int32)
    return (levels, linked)


def draw_levels(key, part):
    return index_table(key)[0]


def draw_neighbours(key, part):
    return index_table(key)[1]


def draw_coupling(key, part):
    first_key, second_key = jax.random.split(jax.random.fold_in(key, 11))
    spread = jax.random.uniform(first_key, (PAIRS, 3, 3), jnp.float32, -0.3, 0.3)
    offdiag = 0.5 * (spread + jnp.swapaxes(spread, 1, 2))
    mainly = jax.random.uniform(second_key, (PAIRS, 3), jnp.float32, 0.8, 1.6)
    identity = jnp.eye(3, dtype=jnp.float32)
    return offdiag * (1.0 - identity) + mainly[:, :, None] * identity


def draw_forcing(key, part):
    keys = jax.random.split(jax.random.fold_in(key, 23), 6)
    shape = (PAIRS, 3, ZMAX, Y, XMAX)
    blocks = ZMAX // ZD
    noise = jnp.clip(jax.random.normal(keys[0], shape, jnp.float32), -4.0, 4.0)
    amplitude = jnp.exp(jax.random.uniform(keys[1], (PAIRS, 1, blocks, 1, 1), jnp.float32, -1.09, 1.09))
    share = jax.random.uniform(keys[2], (PAIRS, 1, blocks, 1, 1), jnp.float32, 0.0, 1.0)
    modes = 6
    magnitude = jax.random.randint(keys[3], (PAIRS, 3, modes, 3), 1, 4, dtype=jnp.int32)
    flipping = 2 * jax.random.randint(keys[4], (PAIRS, 3, modes, 3), 0, 2, dtype=jnp.int32) - 1
    wave = (magnitude * flipping).astype(jnp.float32)
    phase = jax.random.uniform(keys[5], (PAIRS, 3, modes), jnp.float32, 0.0, 2.0 * math.pi)
    along_x = (jnp.arange(XMAX, dtype=jnp.float32) + 0.5) / XMAX
    along_y = (jnp.arange(Y, dtype=jnp.float32) + 0.5) / Y
    along_z = (jnp.arange(ZMAX, dtype=jnp.float32) + 0.5) / ZMAX
    smooth = jnp.zeros(shape, jnp.float32)
    for mode in range(modes):
        angle = wave[:, :, mode, 0][:, :, None, None, None] * along_x[None, None, None, None, :] + wave[:, :, mode, 1][:, :, None, None, None] * along_y[None, None, None, :, None] + wave[:, :, mode, 2][:, :, None, None, None] * along_z[None, None, :, None, None]
        smooth = smooth + jnp.cos(2.0 * math.pi * angle + phase[:, :, mode][:, :, None, None, None])
    smooth = smooth * math.sqrt(2.0 / modes)
    share_rows = jnp.repeat(share, ZD, axis=2)
    amplitude_rows = jnp.repeat(amplitude, ZD, axis=2)
    mixed_field = jnp.sqrt(1.0 - share_rows) * noise + jnp.sqrt(share_rows) * smooth
    return jnp.clip(amplitude_rows * mixed_field, -18.0, 18.0)


def block_scale(stream_key, dims, pieces, low, high):
    loudness, own = 1.0, jax.random.fold_in(stream_key, 6)
    for dim, shards_of in pieces:
        heights = jnp.exp(jax.random.uniform(jax.random.fold_in(own, dim), (shards_of,), jnp.float32, low / len(pieces), high / len(pieces)))
        loudness = loudness * jnp.repeat(heights, dims[dim] // shards_of).reshape([-1 if axis == dim else 1 for axis in range(len(dims))])
    return loudness


def setup_inputs(seed: int = 0) -> dict:
    seeds = jax.random.split(jax.random.key(seed), 7)
    forcing = draw_forcing(jax.random.fold_in(seeds[6], 71), 0)
    stiffness = jnp.clip(jnp.exp(math.log(4.0) - 2.7725887 * jax.random.uniform(seeds[1], (PAIRS, 3, ZMAX, Y, XMAX), jnp.float32) ** block_scale(seeds[1], (PAIRS, 3, ZMAX, Y, XMAX), ((0, 8), (2, 16)), -0.2, 0.2)), 0.25, 4.0)
    anisotropy = jnp.clip(jnp.exp(math.log(3.0) - 2.3025851 * jax.random.uniform(seeds[2], (PAIRS, 3, 3), jnp.float32) ** block_scale(seeds[2], (PAIRS, 3, 3), ((0, 8),), -0.2, 0.2)), 0.3, 3.0)
    coupling = draw_coupling(jax.random.fold_in(seeds[6], 71), 0)
    levels = draw_levels(jax.random.fold_in(seeds[6], 71), 0)
    neighbours = draw_neighbours(jax.random.fold_in(seeds[6], 71), 0)
    return {"forcing": forcing, "stiffness": stiffness, "anisotropy": anisotropy, "coupling": coupling, "levels": levels, "neighbours": neighbours}


def level_factor(level_ids):
    return jnp.where(level_ids == 0, 4, jnp.where(level_ids == 1, 2, 1)).astype(jnp.int32)


def resolution(pair_level):
    cells_x = XMAX // level_factor(pair_level[0])
    run_z = ZD // level_factor(pair_level[1])
    return cells_x, run_z, run_z * N_SLAB


def step_up(values, axis_dim):
    length = values.shape[axis_dim]
    widths = [(0, 0)] * values.ndim
    widths[axis_dim] = (0, 1)
    return lax.slice_in_dim(jnp.pad(values, widths), 1, length + 1, axis=axis_dim)


def step_down(values, axis_dim):
    length = values.shape[axis_dim]
    widths = [(0, 0)] * values.ndim
    widths[axis_dim] = (1, 0)
    return lax.slice_in_dim(jnp.pad(values, widths), 0, length, axis=axis_dim)


def to_grid(stored, run_z):
    row_index = jnp.arange(ZMAX, dtype=jnp.int32)
    source = jnp.minimum((row_index // run_z) * ZD + row_index % run_z, ZMAX - 1)
    return jnp.take(stored, source, axis=1)


def from_grid(grid, run_z):
    row_index = jnp.arange(ZMAX, dtype=jnp.int32)
    inner = row_index % ZD
    source = jnp.minimum((row_index // ZD) * run_z + inner, ZMAX - 1)
    keeping = (inner < run_z).astype(jnp.float32)
    return jnp.take(grid, source, axis=1) * keeping[None, :, None, None]


def operate(values, face_list, coefficient, coupling, active):
    result = jnp.sum(coupling[:, :, None, None, None] * values[None], axis=1)
    for facing in range(3):
        axis_dim = 3 - facing
        upper_face, lower_face = face_list[facing]
        result = result + coefficient[:, facing, None, None, None] * (
            upper_face * (values - step_up(values, axis_dim)) + lower_face * (values - step_down(values, axis_dim)))
    return result * active


def solve_pair(operands):
    forcing, stiffness, anisotropy, coupling, pair_level = operands
    cells_x, run_z, depth_z = resolution(pair_level)
    row_index = jnp.arange(ZMAX, dtype=jnp.int32)
    col_index = jnp.arange(XMAX, dtype=jnp.int32)
    active = ((row_index < depth_z)[:, None, None] & (col_index < cells_x)[None, None, :]).astype(jnp.float32)
    source = to_grid(forcing, run_z) * active
    stiff_grid = to_grid(stiffness, run_z) * active
    scales = jnp.stack([(cells_x.astype(jnp.float32) / Y) ** 2, jnp.ones((), jnp.float32),
                        (depth_z.astype(jnp.float32) / Y) ** 2])
    coefficient = anisotropy * scales[None, :]
    diagonal = jnp.diagonal(coupling)[:, None, None, None]
    face_list = []
    for facing in range(3):
        axis_dim = 3 - facing
        single = stiff_grid[facing:facing + 1]
        upper_face = 0.5 * (single + step_up(single, axis_dim))
        lower_face = 0.5 * (single + step_down(single, axis_dim))
        face_list.append((upper_face, lower_face))
        diagonal = diagonal + coefficient[:, facing, None, None, None] * (upper_face + lower_face)
    residual = source
    precond = residual / diagonal
    search = precond
    solution = jnp.zeros_like(source)
    rz_now = jnp.sum(residual * precond)
    for iteration in range(ITERS):
        applied = operate(search, face_list, coefficient, coupling, active)
        step_size = rz_now / jnp.sum(search * applied)
        solution = solution + step_size * search
        if iteration + 1 < ITERS:
            residual = residual - step_size * applied
            precond = residual / diagonal
            rz_next = jnp.sum(residual * precond)
            search = precond + (rz_next / rz_now) * search
            rz_now = rz_next
    return solution


def two_tap(values, axis_dim, fine, coarse):
    length = values.shape[axis_dim]
    ratio = jnp.maximum(fine // jnp.maximum(coarse, 1), 1)
    cells = jnp.arange(length, dtype=jnp.int32)
    numer = 2 * cells + 1 - ratio
    lowest = jnp.floor_divide(numer, 2 * ratio)
    fraction = (numer - lowest * 2 * ratio).astype(jnp.float32) / (2 * ratio).astype(jnp.float32)
    shaped = [1] * values.ndim
    shaped[axis_dim] = length

    def picked(position):
        valid = ((position >= 0) & (position < coarse)).astype(jnp.float32)
        taken = jnp.take(values, jnp.clip(position, 0, length - 1), axis=axis_dim)
        return taken * valid.reshape(shaped)

    result = (1.0 - fraction).reshape(shaped) * picked(lowest) + fraction.reshape(shaped) * picked(lowest + 1)
    return result * (cells < fine).astype(jnp.float32).reshape(shaped)


def interpolate(values, level_from, level_to):
    x_from, run_from, depth_from = resolution(level_from)
    x_to, run_to, depth_to = resolution(level_to)
    moved = two_tap(values, 3, x_to, x_from)
    return two_tap(moved, 1, depth_to, depth_from)


def reference(forcing, stiffness, anisotropy, coupling, levels, neighbours):
    solved = lax.map(solve_pair, (forcing, stiffness, anisotropy, coupling, levels))

    def mix_pair(position):
        pair_level = levels[position]
        link_ids = neighbours[position]
        result = interpolate(solved[position], pair_level, pair_level)
        for entry, weight_sign in ((0, -1.0), (1, -1.0), (2, 1.0)):
            other_id = jnp.maximum(link_ids[entry], 0)
            other_term = interpolate(solved[other_id], levels[other_id], pair_level)
            result = result + (weight_sign * (link_ids[entry] >= 0).astype(jnp.float32)) * other_term
        return from_grid(result, resolution(pair_level)[1])

    return lax.map(mix_pair, jnp.arange(PAIRS, dtype=jnp.int32))
```

```python
import functools
import jax
import jax.numpy as jnp
from jax import lax
from jax.experimental import pallas as pl
from jax.experimental.pallas import tpu as pltpu
from jax.sharding import PartitionSpec as P

MESH = pl.DeviceIdType.MESH
N_GRP = 8
N_Y = 4
OFFSETS = ((1, 0), (3, 0), (0, 1), (2, 0), (1, 1), (3, 1), (2, 1))
ROWS_UP = (1, 3, 7)


def peer_of(g, dy, dx):
    y, x = g // 2, g % 2
    return ((y + dy) % N_Y) * 2 + (x + dx) % 2


def fold8(v):
    total = v[0:8]
    for i in range(1, v.shape[0] // 8):
        total = total + v[8 * i : 8 * i + 8]
    return total


def body(
    n_s, f_hbm, k_hbm, aniso, coup, levels, neigh, out_hbm,
    f, kk, kz, gx, gy, fz, rj, z0, w, q1, kzup, kza, kzb, up, za, zb, qup, qa, qb,
    pz, pq, rz, rq, ru, corr, rc, ob, acc, mom, momr, tots, tot, cof,
    in_sem, out_sem, ks, kr, zs, zr, qs, qr, ms, mr, ts, tr, pzs, pzr, pqs, pqr, cs, cr,
):
    g = lax.axis_index("grp")
    s = lax.axis_index("slab")
    height, width = f.shape[2], f.shape[3]
    chunk = height // N_GRP
    below_id = (s + n_s - 1) % n_s
    above_id = (s + 1) % n_s

    barrier = pltpu.get_barrier_semaphore()
    for o in range(1, n_s):
        pl.semaphore_signal(barrier, inc=1, device_id={"slab": (s + o) % n_s}, device_id_type=MESH)
    for dy, dx in OFFSETS:
        pl.semaphore_signal(barrier, inc=1, device_id={"grp": peer_of(g, dy, dx)}, device_id_type=MESH)
    load_k = pltpu.make_async_copy(k_hbm.at[0], kk, in_sem.at[0])
    load_f = pltpu.make_async_copy(f_hbm.at[0], f, in_sem.at[1])
    load_k.start()
    load_f.start()

    def sizes(lx, lz):
        nx = jnp.where(lx == 2, width, jnp.where(lx == 1, width // 2, width // 4))
        a = jnp.where(lz == 2, 8, jnp.where(lz == 1, 4, 2))
        return nx, a

    nx, a = sizes(levels[g, 0], levels[g, 1])
    sx = nx.astype(jnp.float32) * (1.0 / height)
    sz = (a * n_s).astype(jnp.float32) * (1.0 / height)
    scale = (sx * sx, 1.0, sz * sz)
    cf = [[aniso[0, c, d] * scale[d] for d in range(3)] for c in range(3)]
    cp = [[coup[0, c, e] for e in range(3)] for c in range(3)]
    sel = [(a == j + 1).astype(jnp.float32) for j in ROWS_UP]
    has_below = (s > 0).astype(jnp.float32)
    has_above = (s < n_s - 1).astype(jnp.float32)

    lane = lax.broadcasted_iota(jnp.int32, (height, width), 1)
    row = lax.broadcasted_iota(jnp.int32, (height, width), 0)
    lane_on = (lane < nx).astype(jnp.float32)

    def top_row(read):
        return sel[0] * read(1) + sel[1] * read(3) + sel[2] * read(7)

    def remote(src, dst, ssem, rsem, device_id):
        return pltpu.make_async_remote_copy(
            src_ref=src, dst_ref=dst, send_sem=ssem, recv_sem=rsem,
            device_id=device_id, device_id_type=MESH,
        )

    def halo(down_src, up_src, above_dst, below_dst, ssem, rsem):
        return (
            remote(down_src, above_dst, ssem.at[0], rsem.at[0], {"slab": below_id}),
            remote(up_src, below_dst, ssem.at[1], rsem.at[1], {"slab": above_id}),
        )

    load_k.wait()
    kzup[...] = top_row(lambda j: kk[2, j])
    pl.semaphore_wait(barrier, n_s - 1 + len(OFFSETS))
    k_halo = halo(kk.at[2, 0], kzup, kza, kzb, ks, kr)
    for cpy in k_halo:
        cpy.start()
    load_f.wait()

    zero = jnp.zeros((height, width), jnp.float32)
    for buf in (z0, q1):
        for c in range(3):
            buf[c, 0] = zero
            buf[c, 9] = zero
    kz[8] = zero
    acc[...] = jnp.zeros_like(acc)

    def faces(k, carry):
        on = lane_on * (k < a).astype(jnp.float32)
        kx = kk[0, k] * on
        ky = kk[1, k] * on
        kz[k] = kk[2, k] * on
        x_up = pltpu.roll(kx, width - 1, 1)
        x_up = jnp.where(lane < width - 1, x_up, 0.0)
        x_down = jnp.where(lane > 0, pltpu.roll(kx, 1, 1), 0.0)
        gx[k] = jnp.where(lane < nx - 1, 0.5 * (kx + x_up), 0.0)
        y_up = jnp.where(row < height - 1, pltpu.roll(ky, height - 1, 0), 0.0)
        y_down = jnp.where(row > 0, pltpu.roll(ky, 1, 0), 0.0)
        gy[k] = jnp.where(row < height - 1, 0.5 * (ky + y_up), 0.0)
        sum_x = kx + 0.5 * (x_up + x_down)
        sum_y = ky + 0.5 * (y_up + y_down)
        for c in range(3):
            rj[c, k] = cp[c][c] + cf[c][0] * sum_x + cf[c][1] * sum_y
            f[c, k] = f[c, k] * on
        return carry

    lax.fori_loop(0, 8, faces, 0)

    for cpy in k_halo:
        cpy.wait()
    fz[0] = 0.5 * (kzb[...] * (lane_on * has_below) + kz[0])
    rim_k = kza[...] * (lane_on * has_above)

    def z_faces(j, carry):
        top = (j == a).astype(jnp.float32)
        fz[j] = 0.5 * (kz[j - 1] + kz[j] + top * rim_k)
        return carry

    lax.fori_loop(1, 9, z_faces, 0)

    def first(k, carry):
        sum_z = fz[k] + fz[k + 1]
        for c in range(3):
            inverse = 1.0 / (rj[c, k] + cf[c][2] * sum_z)
            rj[c, k] = inverse
            fc = f[c, k]
            zc = fc * inverse
            z0[c, k + 1] = zc
            acc[0] += fold8(fc * zc)
        return carry

    lax.fori_loop(0, 8, first, 0)
    for c in range(3):
        up[c] = top_row(lambda j: z0[c, j + 1])
    z_halo = halo(z0.at[:, 1], up, za, zb, zs, zr)
    for cpy in z_halo:
        cpy.start()

    def apply_row(u, base, c, k, values):
        uc = values[c]
        out = base
        for e in range(3):
            if e != c:
                out = out + cp[c][e] * values[e]
        gxk = gx[k]
        gyk = gy[k]
        nb_x = gxk * pltpu.roll(uc, width - 1, 1) + pltpu.roll(gxk * uc, 1, 1)
        nb_y = gyk * pltpu.roll(uc, height - 1, 0) + pltpu.roll(gyk * uc, 1, 0)
        inside = (k < a).astype(jnp.float32)
        nb_z = fz[k + 1] * u[c, k + 2] + (inside * fz[k]) * u[c, k]
        return out - (cf[c][0] * nb_x + cf[c][1] * nb_y + cf[c][2] * nb_z)

    def second(k, carry):
        values = [z0[c, k + 1] for c in range(3)]
        for c in range(3):
            w[c, k] = apply_row(z0, f[c, k], c, k, values)
        return carry

    lax.fori_loop(0, 8, second, 0)
    for cpy in z_halo:
        cpy.wait()
    for c in range(3):
        zb[c] = zb[c] * has_below
        za[c] = za[c] * has_above
        w[c, 0] -= cf[c][2] * (fz[0] * zb[c])
        for i, j in enumerate(ROWS_UP):
            w[c, j] -= (sel[i] * cf[c][2]) * (fz[j + 1] * za[c])

    def third(k, carry):
        for c in range(3):
            wc = w[c, k]
            qc = wc * rj[c, k]
            q1[c, k + 1] = qc
            acc[1] += fold8(z0[c, k + 1] * wc)
            acc[2] += fold8(wc * qc)
        return carry

    lax.fori_loop(0, 8, third, 0)
    for c in range(3):
        qup[c] = top_row(lambda j: q1[c, j + 1])
    q_halo = halo(q1.at[:, 1], qup, qa, qb, qs, qr)
    for cpy in q_halo:
        cpy.start()

    full = (a == 8).astype(jnp.float32)
    part = 1.0 - full

    def pack(u, ua, ub, dst):
        def one(c, carry):
            for r in range(6):
                if r == 0:
                    loose = ub[c]
                elif r == 3:
                    loose = u[c, 3] + sel[0] * ua[c]
                elif r == 5:
                    loose = sel[1] * ua[c]
                else:
                    loose = u[c, r]
                value = part * loose
                if r < 4:
                    value = value + full * (u[c, r + 1] + pltpu.roll(u[c, r + 5], width // 2, 1))
                dst[c, r] = value
            return carry

        lax.fori_loop(0, 3, one, 0)

    def rows_of(i):
        return pl.ds(pl.multiple_of(i * chunk, chunk), chunk)

    def scatter(src, dst, ssem, rsem):
        copies = []
        for o, (dy, dx) in enumerate(OFFSETS):
            to = peer_of(g, dy, dx)
            copies.append(
                remote(src.at[:, :, rows_of(to)], dst.at[g], ssem.at[o], rsem.at[o], {"grp": to})
            )
        return copies

    def await_from(dst, ssem, rsem, o):
        dy, dx = OFFSETS[o]
        source = peer_of(g, N_Y - dy, dx)
        remote(dst.at[source], dst.at[source], ssem.at[o], rsem.at[o], {"grp": source}).wait_recv()

    pack(z0, za, zb, pz)
    z_out = scatter(pz, rz, pzs, pzr)
    for cpy in z_out:
        cpy.start()

    def fourth(k, carry):
        values = [q1[c, k + 1] for c in range(3)]
        for c in range(3):
            acc[3] += fold8(values[c] * apply_row(q1, w[c, k], c, k, values))
        return carry

    lax.fori_loop(0, 8, fourth, 0)
    for cpy in q_halo:
        cpy.wait()
    for c in range(3):
        qb[c] = qb[c] * has_below
        qa[c] = qa[c] * has_above
        cross = q1[c, 1] * (fz[0] * qb[c])
        for i, j in enumerate(ROWS_UP):
            cross = cross + sel[i] * (q1[c, j + 1] * (fz[j + 1] * qa[c]))
        acc[3] -= cf[c][2] * fold8(cross)

    for i in range(4):
        mom[i : i + 1] = jnp.sum(acc[i], axis=0, keepdims=True)
    mom[4:8] = jnp.zeros((4, width), jnp.float32)
    m_out = []
    for o in range(1, n_s):
        to = (s + o) % n_s
        m_out.append(remote(mom, momr.at[s], ms.at[o - 1], mr.at[o - 1], {"slab": to}))
    for cpy in m_out:
        cpy.start()

    pack(q1, qa, qb, pq)
    q_out = scatter(pq, rq, pqs, pqr)
    for cpy in q_out:
        cpy.start()
    momr[s] = mom[...]
    rz[g] = pz[:, :, rows_of(g)]
    rq[g] = pq[:, :, rows_of(g)]

    for o in range(1, n_s):
        source = (s + n_s - o) % n_s
        remote(
            momr.at[source], momr.at[source], ms.at[o - 1], mr.at[o - 1], {"slab": source}
        ).wait_recv()
    total = momr[0]
    for i in range(1, n_s):
        total = total + momr[i]
    tots[...] = total
    t_out = []
    for o, (dy, dx) in enumerate(OFFSETS):
        to = peer_of(g, dy, dx)
        t_out.append(remote(tots, tot.at[g], ts.at[o], tr.at[o], {"grp": to}))
    for cpy in t_out:
        cpy.start()
    tot[g] = tots[...]
    for o in range(len(OFFSETS)):
        await_from(tot, ts, tr, o)
    sums = jnp.sum(tot[...], axis=2, keepdims=True)
    rz0, m1, m2, m3 = (sums[:, i : i + 1] for i in range(4))
    step0 = rz0 / m1
    rz1 = step0 * step0 * m2 - rz0
    beta = rz1 / rz0
    bend = m1 - 2.0 * step0 * m2 + step0 * step0 * m3
    step1 = jnp.clip(rz1 / (bend - beta * rz1 / step0), 0.25, 1024.0)
    cof[0] = jnp.broadcast_to(step0 + step1 * (1.0 + beta), (N_GRP, 8, width))
    cof[1] = jnp.broadcast_to(-step1 * step0, (N_GRP, 8, width))

    for o in range(len(OFFSETS)):
        await_from(rz, pzs, pzr, o)
    for o in range(len(OFFSETS)):
        await_from(rq, pqs, pqr, o)

    def combine(p, carry):
        c0 = jnp.broadcast_to(cof[0, p][0:1], (chunk, width))
        c1 = jnp.broadcast_to(cof[1, p][0:1], (chunk, width))
        for c in range(3):
            for r in range(6):
                ru[p, c, r] = c0 * rz[p, c, r] + c1 * rq[p, c, r]
        return carry

    lax.fori_loop(0, N_GRP, combine, 0)

    lanes = lax.broadcasted_iota(jnp.int32, (chunk, width), 1)
    half = lanes // 2
    beside = jnp.where(lanes % 2 == 1, half + 1, half + (width - 1)) % width
    low = (lanes < width // 2).astype(jnp.float32)

    def mix(t):
        lx, lz = levels[t, 0], levels[t, 1]
        nx_t, a_t = sizes(lx, lz)
        ids = [neigh[t, i] for i in range(3)]
        there = [(i >= 0).astype(jnp.float32) for i in ids]
        n0, n1, n2 = (jnp.maximum(i, 0) for i in ids)
        full_t = (a_t == 8).astype(jnp.float32)
        near = full_t * there[0]
        far = (1.0 - full_t) * there[0]
        on_x = (lanes < nx_t).astype(jnp.float32)

        def one(c, carry):
            for k in range(8):
                m = k // 2
                other = m + 2 * (k % 2)
                if k < 4:
                    v = near * ru[n0, c, k] + far * ru[n0, c, k + 1]
                else:
                    v = near * pltpu.roll(ru[n0, c, k - 4], width // 2, 1)
                v = v * low
                v = v - there[2] * (0.75 * ru[n2, c, m + 1] + 0.25 * ru[n2, c, other])
                x = 0.75 * jnp.take_along_axis(v, half, axis=1) + 0.25 * jnp.take_along_axis(
                    v, beside, axis=1
                )
                x = x + there[1] * (0.75 * ru[n1, c, m + 1] + 0.25 * ru[n1, c, other])
                corr[t, c, k] = x * (on_x * (k < a_t).astype(jnp.float32))
            return carry

        lax.fori_loop(0, 3, one, 0)

    c_out = []
    for o, (dy, dx) in enumerate(OFFSETS):
        to = peer_of(g, dy, dx)
        mix(to)
        cpy = remote(corr.at[to], rc.at[g], cs.at[o], cr.at[o], {"grp": to})
        cpy.start()
        c_out.append(cpy)
    mix(g)
    own0 = jnp.broadcast_to(cof[0, g][0:1], (height, width))
    own1 = jnp.broadcast_to(cof[1, g][0:1], (height, width))

    def own(k, carry):
        for c in range(3):
            ob[c, k] = own0 * z0[c, k + 1] + own1 * q1[c, k + 1]
        return carry

    lax.fori_loop(0, 8, own, 0)

    def finish(source, ref, i):
        rows = rows_of(source)

        def one(k, carry):
            for c in range(3):
                ob[c, k, rows] = ob[c, k, rows] - ref[source, c, k]
            return carry

        lax.fori_loop(0, 8, one, 0)
        cpy = pltpu.make_async_copy(ob.at[:, :, rows], out_hbm.at[0, :, :, rows], out_sem.at[i])
        cpy.start()
        return cpy

    outs = [finish(g, corr, 0)]
    for o, (dy, dx) in enumerate(OFFSETS):
        await_from(rc, cs, cr, o)
        outs.append(finish(peer_of(g, N_Y - dy, dx), rc, o + 1))
    for cpy in z_out + q_out + m_out + t_out + c_out:
        cpy.wait_send()
    for cpy in outs:
        cpy.wait()


def solution(mesh):
    n_s = mesh.shape["slab"]

    def per_device(forcing, stiffness, anisotropy, coupling, levels, neighbours):
        _, _, depth, height, width = forcing.shape
        chunk = height // N_GRP
        plane = (height, width)
        f32 = jnp.float32
        dma = pltpu.SemaphoreType.DMA
        anyspec = pl.BlockSpec(memory_space=pl.ANY)
        smem = pl.BlockSpec(memory_space=pltpu.SMEM)
        vm = lambda *shape: pltpu.VMEM(shape, f32)
        others = len(OFFSETS)
        scratch = [
            vm(3, 8, *plane), vm(3, 8, *plane), vm(9, *plane), vm(8, *plane), vm(8, *plane),
            vm(9, *plane), vm(3, 8, *plane), vm(3, 10, *plane), vm(3, 8, *plane),
            vm(3, 10, *plane),
            vm(*plane), vm(*plane), vm(*plane),
            vm(3, *plane), vm(3, *plane), vm(3, *plane),
            vm(3, *plane), vm(3, *plane), vm(3, *plane),
            vm(3, 6, *plane), vm(3, 6, *plane),
            vm(N_GRP, 3, 6, chunk, width), vm(N_GRP, 3, 6, chunk, width),
            vm(N_GRP, 3, 6, chunk, width),
            vm(N_GRP, 3, 8, chunk, width), vm(N_GRP, 3, 8, chunk, width),
            vm(3, 8, *plane),
            vm(4, 8, width), vm(8, width), vm(n_s, 8, width), vm(8, width),
            vm(N_GRP, 8, width), vm(2, N_GRP, 8, width),
            dma((2,)), dma((N_GRP,)),
            dma((2,)), dma((2,)), dma((2,)), dma((2,)), dma((2,)), dma((2,)),
            dma((n_s - 1,)), dma((n_s - 1,)),
            dma((others,)), dma((others,)), dma((others,)), dma((others,)),
            dma((others,)), dma((others,)), dma((others,)), dma((others,)),
        ]
        return pl.pallas_call(
            functools.partial(body, n_s),
            out_shape=jax.ShapeDtypeStruct(forcing.shape, f32),
            in_specs=[anyspec, anyspec, smem, smem, smem, smem],
            out_specs=anyspec,
            scratch_shapes=scratch,
            compiler_params=pltpu.CompilerParams(
                collective_id=0, has_side_effects=True, vmem_limit_bytes=56 * 1024 * 1024
            ),
        )(forcing, stiffness, anisotropy, coupling, levels, neighbours)

    wide = P("grp", None, "slab", None, None)
    small = P("grp", None, None)
    return jax.shard_map(
        per_device,
        mesh=mesh,
        in_specs=(wide, wide, small, small, P(), P()),
        out_specs=wide,
        check_vma=False,
    )
```

```python
import functools
import jax
import jax.numpy as jnp
from jax import lax
from jax.experimental import pallas as pl
from jax.experimental.pallas import tpu as pltpu
from jax.sharding import PartitionSpec as P

MESH = pl.DeviceIdType.MESH
N_GRP = 8
N_Y = 4
OFFSETS = ((1, 0), (3, 0), (0, 1), (2, 0), (1, 1), (3, 1), (2, 1))
ROWS_UP = (1, 3, 7)


def peer_of(g, dy, dx):
    y, x = g // 2, g % 2
    return ((y + dy) % N_Y) * 2 + (x + dx) % 2


def fold8(v):
    total = v[0:8]
    for i in range(1, v.shape[0] // 8):
        total = total + v[8 * i : 8 * i + 8]
    return total


def body(
    n_s, f_hbm, k_hbm, aniso_hbm, coup_hbm, levels_hbm, neigh_hbm, out,
    aniso, coup, levels, neigh,
    f, kk, kz, gx, gy, fz, rj, z0, w, q1, kzup, kza, kzb, up, za, zb, qup, qa, qb,
    pu, ru, corr, rc, acc, mom, momr,
    in_sem, ks, kr, zs, zr, qs, qr, ms, mr, ps, pr, cs, cr,
):
    g = lax.axis_index("grp")
    s = lax.axis_index("slab")
    height, width = f.shape[2], f.shape[3]
    chunk = height // N_GRP
    below_id = (s + n_s - 1) % n_s
    above_id = (s + 1) % n_s

    barrier = pltpu.get_barrier_semaphore()
    for o in range(1, n_s):
        pl.semaphore_signal(barrier, inc=1, device_id={"slab": (s + o) % n_s}, device_id_type=MESH)
    for dy, dx in OFFSETS:
        pl.semaphore_signal(barrier, inc=1, device_id={"grp": peer_of(g, dy, dx)}, device_id_type=MESH)
    load_k = pltpu.make_async_copy(k_hbm.at[0], kk, in_sem.at[0])
    load_f = pltpu.make_async_copy(f_hbm.at[0], f, in_sem.at[1])
    smalls = [
        pltpu.make_async_copy(src, dst, in_sem.at[2 + i])
        for i, (src, dst) in enumerate(
            ((levels_hbm, levels), (aniso_hbm, aniso), (coup_hbm, coup), (neigh_hbm, neigh))
        )
    ]
    for cpy in smalls:
        cpy.start()
    load_k.start()
    load_f.start()
    for cpy in smalls:
        cpy.wait()

    def sizes(lx, lz):
        nx = jnp.where(lx == 2, width, jnp.where(lx == 1, width // 2, width // 4))
        a = jnp.where(lz == 2, 8, jnp.where(lz == 1, 4, 2))
        return nx, a

    nx, a = sizes(levels[0, g], levels[1, g])
    sx = nx.astype(jnp.float32) * (1.0 / height)
    sz = (a * n_s).astype(jnp.float32) * (1.0 / height)
    scale = (sx * sx, 1.0, sz * sz)
    cf = [[aniso[c, 0, d] * scale[d] for d in range(3)] for c in range(3)]
    cp = [[coup[c, 0, e] for e in range(3)] for c in range(3)]
    sel = [(a == j + 1).astype(jnp.float32) for j in ROWS_UP]
    has_below = (s > 0).astype(jnp.float32)
    has_above = (s < n_s - 1).astype(jnp.float32)

    lane = lax.broadcasted_iota(jnp.int32, (height, width), 1)
    row = lax.broadcasted_iota(jnp.int32, (height, width), 0)
    lane_on = (lane < nx).astype(jnp.float32)

    def top_row(read):
        return sel[0] * read(1) + sel[1] * read(3) + sel[2] * read(7)

    def remote(src, dst, ssem, rsem, device_id):
        return pltpu.make_async_remote_copy(
            src_ref=src, dst_ref=dst, send_sem=ssem, recv_sem=rsem,
            device_id=device_id, device_id_type=MESH,
        )

    def halo(down_src, up_src, above_dst, below_dst, ssem, rsem):
        return (
            remote(down_src, above_dst, ssem.at[0], rsem.at[0], {"slab": below_id}),
            remote(up_src, below_dst, ssem.at[1], rsem.at[1], {"slab": above_id}),
        )

    load_k.wait()
    kzup[...] = top_row(lambda j: kk[2, j])
    pl.semaphore_wait(barrier, n_s - 1 + len(OFFSETS))
    k_halo = halo(kk.at[2, 0], kzup, kza, kzb, ks, kr)
    for cpy in k_halo:
        cpy.start()
    load_f.wait()

    zero = jnp.zeros((height, width), jnp.float32)
    for buf in (z0, q1):
        for c in range(3):
            buf[c, 0] = zero
            buf[c, 9] = zero
    kz[8] = zero
    acc[...] = jnp.zeros_like(acc)

    def faces(k, carry):
        on = lane_on * (k < a).astype(jnp.float32)
        kx = kk[0, k] * on
        ky = kk[1, k] * on
        kz[k] = kk[2, k] * on
        x_up = pltpu.roll(kx, width - 1, 1)
        x_up = jnp.where(lane < width - 1, x_up, 0.0)
        x_down = jnp.where(lane > 0, pltpu.roll(kx, 1, 1), 0.0)
        gx[k] = jnp.where(lane < nx - 1, 0.5 * (kx + x_up), 0.0)
        y_up = jnp.where(row < height - 1, pltpu.roll(ky, height - 1, 0), 0.0)
        y_down = jnp.where(row > 0, pltpu.roll(ky, 1, 0), 0.0)
        gy[k] = jnp.where(row < height - 1, 0.5 * (ky + y_up), 0.0)
        sum_x = kx + 0.5 * (x_up + x_down)
        sum_y = ky + 0.5 * (y_up + y_down)
        for c in range(3):
            rj[c, k] = cp[c][c] + cf[c][0] * sum_x + cf[c][1] * sum_y
            f[c, k] = f[c, k] * on
        return carry

    lax.fori_loop(0, 8, faces, 0)

    for cpy in k_halo:
        cpy.wait()
    fz[0] = 0.5 * (kzb[...] * (lane_on * has_below) + kz[0])
    rim_k = kza[...] * (lane_on * has_above)

    def z_faces(j, carry):
        top = (j == a).astype(jnp.float32)
        fz[j] = 0.5 * (kz[j - 1] + kz[j] + top * rim_k)
        return carry

    lax.fori_loop(1, 9, z_faces, 0)

    def first(k, carry):
        sum_z = fz[k] + fz[k + 1]
        for c in range(3):
            inverse = 1.0 / (rj[c, k] + cf[c][2] * sum_z)
            rj[c, k] = inverse
            fc = f[c, k]
            zc = fc * inverse
            z0[c, k + 1] = zc
            acc[0] += fold8(fc * zc)
        return carry

    lax.fori_loop(0, 8, first, 0)
    for c in range(3):
        up[c] = top_row(lambda j: z0[c, j + 1])
    z_halo = halo(z0.at[:, 1], up, za, zb, zs, zr)
    for cpy in z_halo:
        cpy.start()

    def apply_row(u, base, c, k, values):
        uc = values[c]
        out = base
        for e in range(3):
            if e != c:
                out = out + cp[c][e] * values[e]
        gxk = gx[k]
        gyk = gy[k]
        nb_x = gxk * pltpu.roll(uc, width - 1, 1) + pltpu.roll(gxk * uc, 1, 1)
        nb_y = gyk * pltpu.roll(uc, height - 1, 0) + pltpu.roll(gyk * uc, 1, 0)
        inside = (k < a).astype(jnp.float32)
        nb_z = fz[k + 1] * u[c, k + 2] + (inside * fz[k]) * u[c, k]
        return out - (cf[c][0] * nb_x + cf[c][1] * nb_y + cf[c][2] * nb_z)

    def second(k, carry):
        values = [z0[c, k + 1] for c in range(3)]
        for c in range(3):
            w[c, k] = apply_row(z0, f[c, k], c, k, values)
        return carry

    lax.fori_loop(0, 8, second, 0)
    for cpy in z_halo:
        cpy.wait()
    for c in range(3):
        zb[c] = zb[c] * has_below
        za[c] = za[c] * has_above
        w[c, 0] -= cf[c][2] * (fz[0] * zb[c])
        for i, j in enumerate(ROWS_UP):
            w[c, j] -= (sel[i] * cf[c][2]) * (fz[j + 1] * za[c])

    def third(k, carry):
        for c in range(3):
            wc = w[c, k]
            qc = wc * rj[c, k]
            q1[c, k + 1] = qc
            acc[1] += fold8(z0[c, k + 1] * wc)
            acc[2] += fold8(wc * qc)
        return carry

    lax.fori_loop(0, 8, third, 0)
    for c in range(3):
        qup[c] = top_row(lambda j: q1[c, j + 1])
    q_halo = halo(q1.at[:, 1], qup, qa, qb, qs, qr)
    for cpy in q_halo:
        cpy.start()

    full = (a == 8).astype(jnp.float32)
    part = 1.0 - full

    def rows_of(i):
        return pl.ds(pl.multiple_of(i * chunk, chunk), chunk)

    def scatter(src, dst, ssem, rsem):
        copies = []
        for o, (dy, dx) in enumerate(OFFSETS):
            to = peer_of(g, dy, dx)
            copies.append(
                remote(src.at[:, :, rows_of(to)], dst.at[g], ssem.at[o], rsem.at[o], {"grp": to})
            )
        return copies

    def await_from(dst, ssem, rsem, o):
        dy, dx = OFFSETS[o]
        source = peer_of(g, N_Y - dy, dx)
        remote(dst.at[source], dst.at[source], ssem.at[o], rsem.at[o], {"grp": source}).wait_recv()

    def fourth(k, carry):
        values = [q1[c, k + 1] for c in range(3)]
        for c in range(3):
            acc[3] += fold8(values[c] * apply_row(q1, w[c, k], c, k, values))
        return carry

    lax.fori_loop(0, 8, fourth, 0)
    for cpy in q_halo:
        cpy.wait()
    for c in range(3):
        qb[c] = qb[c] * has_below
        qa[c] = qa[c] * has_above
        cross = q1[c, 1] * (fz[0] * qb[c])
        for i, j in enumerate(ROWS_UP):
            cross = cross + sel[i] * (q1[c, j + 1] * (fz[j + 1] * qa[c]))
        acc[3] -= cf[c][2] * fold8(cross)

    for i in range(4):
        mom[i : i + 1] = jnp.sum(acc[i], axis=0, keepdims=True)
    mom[4:8] = jnp.zeros((4, width), jnp.float32)
    m_out = []
    for o in range(1, n_s):
        to = (s + o) % n_s
        m_out.append(remote(mom, momr.at[s], ms.at[o - 1], mr.at[o - 1], {"slab": to}))
    for cpy in m_out:
        cpy.start()

    momr[s] = mom[...]
    for o in range(1, n_s):
        source = (s + n_s - o) % n_s
        remote(
            momr.at[source], momr.at[source], ms.at[o - 1], mr.at[o - 1], {"slab": source}
        ).wait_recv()
    total = momr[0]
    for i in range(1, n_s):
        total = total + momr[i]
    sums = jnp.sum(total, axis=1, keepdims=True)
    rz0, m1, m2, m3 = (sums[i : i + 1] for i in range(4))
    step0 = rz0 / m1
    rz1 = step0 * step0 * m2 - rz0
    beta = rz1 / rz0
    bend = m1 - 2.0 * step0 * m2 + step0 * step0 * m3
    step1 = jnp.clip(rz1 / (bend - beta * rz1 / step0), 0.25, 1024.0)
    on_z = jnp.broadcast_to(step0 + step1 * (1.0 + beta), (height, width))
    on_q = jnp.broadcast_to(-step1 * step0, (height, width))

    def solve(c, carry):
        rows = [on_z * z0[c, k + 1] + on_q * q1[c, k + 1] for k in range(8)]
        rim_below = on_z * zb[c] + on_q * qb[c]
        rim_above = on_z * za[c] + on_q * qa[c]
        for k in range(8):
            out[0, c, k] = rows[k]
        for r in range(6):
            if r == 0:
                value = part * rim_below
            elif r == 3:
                value = part * (rows[2] + sel[0] * rim_above)
            elif r == 5:
                value = sel[1] * rim_above
            else:
                value = part * rows[r - 1]
            if r < 4:
                value = value + full * (rows[r] + pltpu.roll(rows[r + 4], width // 2, 1))
            pu[c, r] = value
        return carry

    lax.fori_loop(0, 3, solve, 0)
    p_out = scatter(pu, ru, ps, pr)
    for cpy in p_out:
        cpy.start()
    ru[g] = pu[:, :, rows_of(g)]
    for o in range(len(OFFSETS)):
        await_from(ru, ps, pr, o)

    lanes = lax.broadcasted_iota(jnp.int32, (chunk, width), 1)
    half = lanes // 2
    beside = jnp.where(lanes % 2 == 1, half + 1, half + (width - 1)) % width
    low = (lanes < width // 2).astype(jnp.float32)

    def mix(t):
        lx, lz = levels[0, t], levels[1, t]
        nx_t, a_t = sizes(lx, lz)
        ids = [neigh[i, t] for i in range(3)]
        there = [(i >= 0).astype(jnp.float32) for i in ids]
        n0, n1, n2 = (jnp.maximum(i, 0) for i in ids)
        full_t = (a_t == 8).astype(jnp.float32)
        near = full_t * there[0]
        far = (1.0 - full_t) * there[0]
        on_x = (lanes < nx_t).astype(jnp.float32)

        def one(c, carry):
            for k in range(8):
                m = k // 2
                other = m + 2 * (k % 2)
                if k < 4:
                    v = near * ru[n0, c, k] + far * ru[n0, c, k + 1]
                else:
                    v = near * pltpu.roll(ru[n0, c, k - 4], width // 2, 1)
                v = v * low
                v = v - there[2] * (0.75 * ru[n2, c, m + 1] + 0.25 * ru[n2, c, other])
                x = 0.75 * jnp.take_along_axis(v, half, axis=1) + 0.25 * jnp.take_along_axis(
                    v, beside, axis=1
                )
                x = x + there[1] * (0.75 * ru[n1, c, m + 1] + 0.25 * ru[n1, c, other])
                corr[t, c, k] = x * (on_x * (k < a_t).astype(jnp.float32))
            return carry

        lax.fori_loop(0, 3, one, 0)

    c_out = []
    for o, (dy, dx) in enumerate(OFFSETS):
        to = peer_of(g, dy, dx)
        mix(to)
        cpy = remote(corr.at[to], rc.at[g], cs.at[o], cr.at[o], {"grp": to})
        cpy.start()
        c_out.append(cpy)
    mix(g)

    def finish(source, ref):
        rows = rows_of(source)

        def one(k, carry):
            for c in range(3):
                out[0, c, k, rows] = out[0, c, k, rows] - ref[source, c, k]
            return carry

        lax.fori_loop(0, 8, one, 0)

    finish(g, corr)
    for o, (dy, dx) in enumerate(OFFSETS):
        await_from(rc, cs, cr, o)
        finish(peer_of(g, N_Y - dy, dx), rc)
    for cpy in m_out + p_out + c_out:
        cpy.wait_send()


def solution(mesh):
    n_s = mesh.shape["slab"]

    def per_device(forcing, stiffness, anisotropy, coupling, levels, neighbours):
        _, _, depth, height, width = forcing.shape
        anisotropy = jnp.transpose(anisotropy, (1, 0, 2))
        coupling = jnp.transpose(coupling, (1, 0, 2))
        levels = levels.T
        neighbours = neighbours.T
        chunk = height // N_GRP
        plane = (height, width)
        f32 = jnp.float32
        dma = pltpu.SemaphoreType.DMA
        anyspec = pl.BlockSpec(memory_space=pl.ANY)
        vm = lambda *shape: pltpu.VMEM(shape, f32)
        others = len(OFFSETS)
        scratch = [
            pltpu.SMEM(anisotropy.shape, f32), pltpu.SMEM(coupling.shape, f32),
            pltpu.SMEM(levels.shape, jnp.int32), pltpu.SMEM(neighbours.shape, jnp.int32),
            vm(3, 8, *plane), vm(3, 8, *plane), vm(9, *plane), vm(8, *plane), vm(8, *plane),
            vm(9, *plane), vm(3, 8, *plane), vm(3, 10, *plane), vm(3, 8, *plane),
            vm(3, 10, *plane),
            vm(*plane), vm(*plane), vm(*plane),
            vm(3, *plane), vm(3, *plane), vm(3, *plane),
            vm(3, *plane), vm(3, *plane), vm(3, *plane),
            vm(3, 6, *plane), vm(N_GRP, 3, 6, chunk, width),
            vm(N_GRP, 3, 8, chunk, width), vm(N_GRP, 3, 8, chunk, width),
            vm(4, 8, width), vm(8, width), vm(n_s, 8, width),
            dma((6,)),
            dma((2,)), dma((2,)), dma((2,)), dma((2,)), dma((2,)), dma((2,)),
            dma((n_s - 1,)), dma((n_s - 1,)),
            dma((others,)), dma((others,)), dma((others,)), dma((others,)),
        ]
        return pl.pallas_call(
            functools.partial(body, n_s),
            out_shape=pltpu.VMEM(forcing.shape, f32),
            in_specs=[anyspec] * 6,
            out_specs=pl.BlockSpec(memory_space=pltpu.VMEM),
            scratch_shapes=scratch,
            compiler_params=pltpu.CompilerParams(
                collective_id=0, has_side_effects=True, vmem_limit_bytes=56 * 1024 * 1024
            ),
        )(forcing, stiffness, anisotropy, coupling, levels, neighbours)

    wide = P("grp", None, "slab", None, None)
    small = P("grp", None, None)
    return jax.shard_map(
        per_device,
        mesh=mesh,
        in_specs=(wide, wide, small, small, P(), P()),
        out_specs=wide,
        check_vma=False,
    )
```

```python
import functools
import jax
import jax.numpy as jnp
from jax import lax
from jax.experimental import pallas as pl
from jax.experimental.pallas import tpu as pltpu
from jax.sharding import PartitionSpec as P

MESH = pl.DeviceIdType.MESH
N_GRP = 8
N_Y = 4
OFFSETS = ((1, 0), (3, 0), (0, 1), (2, 0), (1, 1), (3, 1), (2, 1))
ROWS_UP = (1, 3, 7)


def peer_of(g, dy, dx):
    y, x = g // 2, g % 2
    return ((y + dy) % N_Y) * 2 + (x + dx) % 2


def fold8(v):
    total = v[0:8]
    for i in range(1, v.shape[0] // 8):
        total = total + v[8 * i : 8 * i + 8]
    return total


def body(
    n_s, f_hbm, k_hbm, aniso_hbm, coup_hbm, levels_hbm, neigh_hbm, out,
    aniso, coup, levels, neigh,
    f, kk, kz, gx, gy, fz, rj, z0, w, q1, kzup, kza, kzb, up, za, zb, qup, qa, qb,
    pu, ru0, ru1, ru2, corr, rc, acc, mom, momr,
    in_sem, ks, kr, zs, zr, qs, qr, ms, mr, ps, pr, cs, cr,
):
    g = lax.axis_index("grp")
    s = lax.axis_index("slab")
    height, width = f.shape[2], f.shape[3]
    chunk = height // N_GRP
    below_id = (s + n_s - 1) % n_s
    above_id = (s + 1) % n_s

    ru = (ru0, ru1, ru2)

    barrier = pltpu.get_barrier_semaphore()
    for o in range(1, n_s):
        pl.semaphore_signal(barrier, inc=1, device_id={"slab": (s + o) % n_s}, device_id_type=MESH)
    for dy, dx in OFFSETS:
        pl.semaphore_signal(barrier, inc=1, device_id={"grp": peer_of(g, dy, dx)}, device_id_type=MESH)
    load_k = pltpu.make_async_copy(k_hbm.at[0], kk, in_sem.at[0])
    load_f = pltpu.make_async_copy(f_hbm.at[0], f, in_sem.at[1])
    smalls = [
        pltpu.make_async_copy(src, dst, in_sem.at[2 + i])
        for i, (src, dst) in enumerate(
            ((levels_hbm, levels), (aniso_hbm, aniso), (coup_hbm, coup), (neigh_hbm, neigh))
        )
    ]
    for cpy in smalls:
        cpy.start()
    load_k.start()
    load_f.start()
    for cpy in smalls:
        cpy.wait()

    def sizes(lx, lz):
        nx = jnp.where(lx == 2, width, jnp.where(lx == 1, width // 2, width // 4))
        a = jnp.where(lz == 2, 8, jnp.where(lz == 1, 4, 2))
        return nx, a

    nx, a = sizes(levels[0, g], levels[1, g])
    sx = nx.astype(jnp.float32) * (1.0 / height)
    sz = (a * n_s).astype(jnp.float32) * (1.0 / height)
    scale = (sx * sx, 1.0, sz * sz)
    cf = [[aniso[c, 0, d] * scale[d] for d in range(3)] for c in range(3)]
    cp = [[coup[c, 0, e] for e in range(3)] for c in range(3)]
    sel = [(a == j + 1).astype(jnp.float32) for j in ROWS_UP]
    has_below = (s > 0).astype(jnp.float32)
    has_above = (s < n_s - 1).astype(jnp.float32)

    lane = lax.broadcasted_iota(jnp.int32, (height, width), 1)
    row = lax.broadcasted_iota(jnp.int32, (height, width), 0)
    lane_on = (lane < nx).astype(jnp.float32)

    def top_row(read):
        return sel[0] * read(1) + sel[1] * read(3) + sel[2] * read(7)

    def remote(src, dst, ssem, rsem, device_id):
        return pltpu.make_async_remote_copy(
            src_ref=src, dst_ref=dst, send_sem=ssem, recv_sem=rsem,
            device_id=device_id, device_id_type=MESH,
        )

    def halo(down_src, up_src, above_dst, below_dst, ssem, rsem):
        return (
            remote(down_src, above_dst, ssem.at[0], rsem.at[0], {"slab": below_id}),
            remote(up_src, below_dst, ssem.at[1], rsem.at[1], {"slab": above_id}),
        )

    load_k.wait()
    kzup[...] = top_row(lambda j: kk[2, j])
    pl.semaphore_wait(barrier, n_s - 1 + len(OFFSETS))
    k_halo = halo(kk.at[2, 0], kzup, kza, kzb, ks, kr)
    for cpy in k_halo:
        cpy.start()
    load_f.wait()

    zero = jnp.zeros((height, width), jnp.float32)
    for buf in (z0, q1):
        for c in range(3):
            buf[c, 0] = zero
            buf[c, 9] = zero
    kz[8] = zero
    acc[...] = jnp.zeros_like(acc)

    def faces(k, carry):
        on = lane_on * (k < a).astype(jnp.float32)
        kx = kk[0, k] * on
        ky = kk[1, k] * on
        kz[k] = kk[2, k] * on
        x_up = pltpu.roll(kx, width - 1, 1)
        x_up = jnp.where(lane < width - 1, x_up, 0.0)
        x_down = jnp.where(lane > 0, pltpu.roll(kx, 1, 1), 0.0)
        gx[k] = jnp.where(lane < nx - 1, 0.5 * (kx + x_up), 0.0)
        y_up = jnp.where(row < height - 1, pltpu.roll(ky, height - 1, 0), 0.0)
        y_down = jnp.where(row > 0, pltpu.roll(ky, 1, 0), 0.0)
        gy[k] = jnp.where(row < height - 1, 0.5 * (ky + y_up), 0.0)
        sum_x = kx + 0.5 * (x_up + x_down)
        sum_y = ky + 0.5 * (y_up + y_down)
        for c in range(3):
            rj[c, k] = cp[c][c] + cf[c][0] * sum_x + cf[c][1] * sum_y
            f[c, k] = f[c, k] * on
        return carry

    lax.fori_loop(0, 8, faces, 0)

    for cpy in k_halo:
        cpy.wait()
    fz[0] = 0.5 * (kzb[...] * (lane_on * has_below) + kz[0])
    rim_k = kza[...] * (lane_on * has_above)

    def z_faces(j, carry):
        top = (j == a).astype(jnp.float32)
        fz[j] = 0.5 * (kz[j - 1] + kz[j] + top * rim_k)
        return carry

    lax.fori_loop(1, 9, z_faces, 0)

    def jacobi(c, k):
        return f[c, k] * (1.0 / (rj[c, k] + cf[c][2] * (fz[k] + fz[k + 1])))

    for c in range(3):
        z0[c, 1] = jacobi(c, 0)
        up[c] = jacobi(c, a - 1)
    z_halo = halo(z0.at[:, 1], up, za, zb, zs, zr)
    for cpy in z_halo:
        cpy.start()

    def invert(k):
        sum_z = fz[k] + fz[k + 1]
        for c in range(3):
            rj[c, k] = 1.0 / (rj[c, k] + cf[c][2] * sum_z)

    def first(k, carry):
        invert(k)
        for c in range(3):
            fc = f[c, k]
            zc = fc * rj[c, k]
            z0[c, k + 1] = zc
            acc[0] += fold8(fc * zc)
        return carry

    invert(0)
    for c in range(3):
        acc[0] += fold8(f[c, 0] * z0[c, 1])
    lax.fori_loop(1, 8, first, 0)

    def apply_row(u, base, c, k, values):
        uc = values[c]
        out = base
        for e in range(3):
            if e != c:
                out = out + cp[c][e] * values[e]
        gxk = gx[k]
        gyk = gy[k]
        nb_x = gxk * pltpu.roll(uc, width - 1, 1) + pltpu.roll(gxk * uc, 1, 1)
        nb_y = gyk * pltpu.roll(uc, height - 1, 0) + pltpu.roll(gyk * uc, 1, 0)
        inside = (k < a).astype(jnp.float32)
        nb_z = fz[k + 1] * u[c, k + 2] + (inside * fz[k]) * u[c, k]
        return out - (cf[c][0] * nb_x + cf[c][1] * nb_y + cf[c][2] * nb_z)

    def second(k, carry):
        values = [z0[c, k + 1] for c in range(3)]
        for c in range(3):
            w[c, k] = apply_row(z0, f[c, k], c, k, values)
        return carry

    lax.fori_loop(0, 8, second, 0)
    for cpy in z_halo:
        cpy.wait()
    for c in range(3):
        zb[c] = zb[c] * has_below
        wc = w[c, 0] - cf[c][2] * (fz[0] * zb[c])
        w[c, 0] = wc
        q1[c, 1] = wc * rj[c, 0]
    q_down = remote(q1.at[:, 1], qa, qs.at[0], qr.at[0], {"slab": below_id})
    q_down.start()
    for c in range(3):
        za[c] = za[c] * has_above
        for i, j in enumerate(ROWS_UP):
            w[c, j] -= (sel[i] * cf[c][2]) * (fz[j + 1] * za[c])

    def sums_of(c, k, qc):
        wc = w[c, k]
        acc[1] += fold8(z0[c, k + 1] * wc)
        acc[2] += fold8(wc * qc)

    def third(k, carry):
        for c in range(3):
            qc = w[c, k] * rj[c, k]
            q1[c, k + 1] = qc
            sums_of(c, k, qc)
        return carry

    for c in range(3):
        sums_of(c, 0, q1[c, 1])
    lax.fori_loop(1, 8, third, 0)
    for c in range(3):
        qup[c] = top_row(lambda j: q1[c, j + 1])

    full = (a == 8).astype(jnp.float32)
    part = 1.0 - full

    def rows_of(i):
        return pl.ds(pl.multiple_of(i * chunk, chunk), chunk)

    def await_from(dst, c, ssem, rsem, o):
        dy, dx = OFFSETS[o]
        source = peer_of(g, N_Y - dy, dx)
        ref = dst(source, c)
        remote(ref, ref, ssem.at[c, o], rsem.at[c, o], {"grp": source}).wait_recv()
        return source

    def fourth(k, carry):
        values = [q1[c, k + 1] for c in range(3)]
        for c in range(3):
            acc[3] += fold8(values[c] * apply_row(q1, w[c, k], c, k, values))
        return carry

    lax.fori_loop(0, 8, fourth, 0)
    fz_top = top_row(lambda j: fz[j + 1]) * (2.0 * has_above)
    q_down.wait()
    for c in range(3):
        acc[3] -= cf[c][2] * fold8(qup[c] * (fz_top * qa[c]))

    for i in range(4):
        mom[i : i + 1] = jnp.sum(acc[i], axis=0, keepdims=True)
    mom[4:8] = jnp.zeros((4, width), jnp.float32)
    m_out = []
    for o in range(1, n_s):
        to = (s + o) % n_s
        m_out.append(remote(mom, momr.at[s], ms.at[o - 1], mr.at[o - 1], {"slab": to}))
    for cpy in m_out:
        cpy.start()
    q_up = remote(qup, qb, qs.at[1], qr.at[1], {"slab": above_id})
    q_up.start()
    momr[s] = mom[...]
    for o in range(1, n_s):
        source = (s + n_s - o) % n_s
        remote(
            momr.at[source], momr.at[source], ms.at[o - 1], mr.at[o - 1], {"slab": source}
        ).wait_recv()
    total = momr[0]
    for i in range(1, n_s):
        total = total + momr[i]
    sums = jnp.sum(total, axis=1, keepdims=True)
    rz0, m1, m2, m3 = (sums[i : i + 1] for i in range(4))
    step0 = rz0 / m1
    rz1 = step0 * step0 * m2 - rz0
    beta = rz1 / rz0
    bend = m1 - 2.0 * step0 * m2 + step0 * step0 * m3
    step1 = jnp.clip(rz1 / (bend - beta * rz1 / step0), 0.25, 1024.0)
    on_z = jnp.broadcast_to(step0 + step1 * (1.0 + beta), (height, width))
    on_q = jnp.broadcast_to(-step1 * step0, (height, width))

    q_up.wait()
    p_out = []
    for c in range(3):
        rows = [on_z * z0[c, k + 1] + on_q * q1[c, k + 1] for k in range(8)]
        rim_below = on_z * zb[c] + on_q * (qb[c] * has_below)
        rim_above = on_z * za[c] + on_q * (qa[c] * has_above)
        for r in range(6):
            if r == 0:
                value = part * rim_below
            elif r == 3:
                value = part * (rows[2] + sel[0] * rim_above)
            elif r == 5:
                value = sel[1] * rim_above
            else:
                value = part * rows[r - 1]
            if r < 4:
                value = value + full * (rows[r] + pltpu.roll(rows[r + 4], width // 2, 1))
            pu[c, r] = value
        for o, (dy, dx) in enumerate(OFFSETS):
            to = peer_of(g, dy, dx)
            cpy = remote(
                pu.at[c, :, rows_of(to)], ru[c].at[g], ps.at[c, o], pr.at[c, o], {"grp": to}
            )
            cpy.start()
            p_out.append(cpy)
        for k in range(8):
            out[0, c, k] = rows[k]
        ru[c][g] = pu[c, :, rows_of(g)]

    lanes = lax.broadcasted_iota(jnp.int32, (chunk, width), 1)
    half = lanes // 2
    beside = jnp.where(lanes % 2 == 1, half + 1, half + (width - 1)) % width
    low = (lanes < width // 2).astype(jnp.float32)

    def mix(t, c):
        lx, lz = levels[0, t], levels[1, t]
        nx_t, a_t = sizes(lx, lz)
        ids = [neigh[i, t] for i in range(3)]
        there = [(i >= 0).astype(jnp.float32) for i in ids]
        n0, n1, n2 = (jnp.maximum(i, 0) for i in ids)
        full_t = (a_t == 8).astype(jnp.float32)
        near = full_t * there[0]
        far = (1.0 - full_t) * there[0]
        on_x = (lanes < nx_t).astype(jnp.float32)
        for k in range(8):
            m = k // 2
            other = m + 2 * (k % 2)
            if k < 4:
                v = near * ru[c][n0, k] + far * ru[c][n0, k + 1]
            else:
                v = near * pltpu.roll(ru[c][n0, k - 4], width // 2, 1)
            v = v * low
            v = v - there[2] * (0.75 * ru[c][n2, m + 1] + 0.25 * ru[c][n2, other])
            x = 0.75 * jnp.take_along_axis(v, half, axis=1) + 0.25 * jnp.take_along_axis(
                v, beside, axis=1
            )
            x = x + there[1] * (0.75 * ru[c][n1, m + 1] + 0.25 * ru[c][n1, other])
            corr[t, c, k] = x * (on_x * (k < a_t).astype(jnp.float32))

    def finish(source, c, ref):
        rows = rows_of(source)
        for k in range(8):
            out[0, c, k, rows] = out[0, c, k, rows] - ref[source, c, k]

    c_out = []
    for c in range(3):
        for o in range(len(OFFSETS)):
            await_from(lambda i, j: ru[j].at[i], c, ps, pr, o)
        for o, (dy, dx) in enumerate(OFFSETS):
            to = peer_of(g, dy, dx)
            mix(to, c)
            cpy = remote(corr.at[to, c], rc.at[g, c], cs.at[c, o], cr.at[c, o], {"grp": to})
            cpy.start()
            c_out.append(cpy)
        mix(g, c)
        finish(g, c, corr)
    for c in range(3):
        for o in range(len(OFFSETS)):
            finish(await_from(lambda i, j: rc.at[i, j], c, cs, cr, o), c, rc)
    for cpy in m_out + p_out + c_out:
        cpy.wait_send()


def solution(mesh):
    n_s = mesh.shape["slab"]

    def per_device(forcing, stiffness, anisotropy, coupling, levels, neighbours):
        _, _, depth, height, width = forcing.shape
        anisotropy = jnp.transpose(anisotropy, (1, 0, 2))
        coupling = jnp.transpose(coupling, (1, 0, 2))
        levels = levels.T
        neighbours = neighbours.T
        chunk = height // N_GRP
        plane = (height, width)
        f32 = jnp.float32
        dma = pltpu.SemaphoreType.DMA
        anyspec = pl.BlockSpec(memory_space=pl.ANY)
        vm = lambda *shape: pltpu.VMEM(shape, f32)
        others = len(OFFSETS)
        scratch = [
            pltpu.SMEM(anisotropy.shape, f32), pltpu.SMEM(coupling.shape, f32),
            pltpu.SMEM(levels.shape, jnp.int32), pltpu.SMEM(neighbours.shape, jnp.int32),
            vm(3, 8, *plane), vm(3, 8, *plane), vm(9, *plane), vm(8, *plane), vm(8, *plane),
            vm(9, *plane), vm(3, 8, *plane), vm(3, 10, *plane), vm(3, 8, *plane),
            vm(3, 10, *plane),
            vm(*plane), vm(*plane), vm(*plane),
            vm(3, *plane), vm(3, *plane), vm(3, *plane),
            vm(3, *plane), vm(3, *plane), vm(3, *plane),
            vm(3, 6, *plane), *(vm(N_GRP, 6, chunk, width) for _ in range(3)),
            vm(N_GRP, 3, 8, chunk, width), vm(N_GRP, 3, 8, chunk, width),
            vm(4, 8, width), vm(8, width), vm(n_s, 8, width),
            dma((6,)),
            dma((2,)), dma((2,)), dma((2,)), dma((2,)), dma((2,)), dma((2,)),
            dma((n_s - 1,)), dma((n_s - 1,)),
            dma((3, others)), dma((3, others)), dma((3, others)), dma((3, others)),
        ]
        return pl.pallas_call(
            functools.partial(body, n_s),
            out_shape=pltpu.VMEM(forcing.shape, f32),
            in_specs=[anyspec] * 6,
            out_specs=pl.BlockSpec(memory_space=pltpu.VMEM),
            scratch_shapes=scratch,
            compiler_params=pltpu.CompilerParams(
                collective_id=0, has_side_effects=True, vmem_limit_bytes=56 * 1024 * 1024
            ),
        )(forcing, stiffness, anisotropy, coupling, levels, neighbours)

    wide = P("grp", None, "slab", None, None)
    small = P("grp", None, None)
    return jax.shard_map(
        per_device,
        mesh=mesh,
        in_specs=(wide, wide, small, small, P(), P()),
        out_specs=wide,
        check_vma=False,
    )
```

```python
import functools
import jax
import jax.numpy as jnp
from jax import lax
from jax.experimental import pallas as pl
from jax.experimental.pallas import tpu as pltpu
from jax.sharding import PartitionSpec as P

MESH = pl.DeviceIdType.MESH
N_GRP = 8
N_Y = 4
OFFSETS = ((1, 0), (3, 0), (0, 1), (2, 0), (1, 1), (3, 1), (2, 1))
ROWS_UP = (1, 3, 7)


def peer_of(g, dy, dx):
    y, x = g // 2, g % 2
    return ((y + dy) % N_Y) * 2 + (x + dx) % 2


def fold8(v):
    total = v[0:8]
    for i in range(1, v.shape[0] // 8):
        total = total + v[8 * i : 8 * i + 8]
    return total


def body(
    n_s, f_hbm, k_hbm, aniso_hbm, coup_hbm, levels_hbm, neigh_hbm, out,
    aniso, coup, levels, neigh,
    f, kk, kz, gx, gy, fz, rj, z0, w, q1, kzup, kza, kzb, up, za, zb, qup, qa, qb,
    pu, rim, rims, ru0, ru1, ru2, si0, si1, si2, ri0, ri1, ri2, corr, rc, acc, mom, momr,
    in_sem, ks, kr, zs, zr, qs, qr, ms, mr, ps, pr, rs, rr, ds, dr, cs, cr,
):
    g = lax.axis_index("grp")
    s = lax.axis_index("slab")
    height, width = f.shape[2], f.shape[3]
    chunk = height // N_GRP
    below_id = (s + n_s - 1) % n_s
    above_id = (s + 1) % n_s

    ru = (ru0, ru1, ru2)
    inner_out = (si0, si1, si2)
    inner = (ri0, ri1, ri2)

    barrier = pltpu.get_barrier_semaphore()
    for o in range(1, n_s):
        pl.semaphore_signal(barrier, inc=1, device_id={"slab": (s + o) % n_s}, device_id_type=MESH)
    for dy, dx in OFFSETS:
        pl.semaphore_signal(barrier, inc=1, device_id={"grp": peer_of(g, dy, dx)}, device_id_type=MESH)
    load_k = pltpu.make_async_copy(k_hbm.at[0], kk, in_sem.at[0])
    load_f = pltpu.make_async_copy(f_hbm.at[0], f, in_sem.at[1])
    smalls = [
        pltpu.make_async_copy(src, dst, in_sem.at[2 + i])
        for i, (src, dst) in enumerate(
            ((levels_hbm, levels), (aniso_hbm, aniso), (coup_hbm, coup), (neigh_hbm, neigh))
        )
    ]
    for cpy in smalls:
        cpy.start()
    load_k.start()
    load_f.start()
    for cpy in smalls:
        cpy.wait()

    def sizes(lx, lz):
        nx = jnp.where(lx == 2, width, jnp.where(lx == 1, width // 2, width // 4))
        a = jnp.where(lz == 2, 8, jnp.where(lz == 1, 4, 2))
        return nx, a

    nx, a = sizes(levels[0, g], levels[1, g])
    sx = nx.astype(jnp.float32) * (1.0 / height)
    sz = (a * n_s).astype(jnp.float32) * (1.0 / height)
    scale = (sx * sx, 1.0, sz * sz)
    cf = [[aniso[c, 0, d] * scale[d] for d in range(3)] for c in range(3)]
    cp = [[coup[c, 0, e] for e in range(3)] for c in range(3)]
    sel = [(a == j + 1).astype(jnp.float32) for j in ROWS_UP]
    has_below = (s > 0).astype(jnp.float32)
    has_above = (s < n_s - 1).astype(jnp.float32)

    lane = lax.broadcasted_iota(jnp.int32, (height, width), 1)
    row = lax.broadcasted_iota(jnp.int32, (height, width), 0)
    lane_on = (lane < nx).astype(jnp.float32)

    def top_row(read):
        return sel[0] * read(1) + sel[1] * read(3) + sel[2] * read(7)

    def remote(src, dst, ssem, rsem, device_id):
        return pltpu.make_async_remote_copy(
            src_ref=src, dst_ref=dst, send_sem=ssem, recv_sem=rsem,
            device_id=device_id, device_id_type=MESH,
        )

    def halo(down_src, up_src, above_dst, below_dst, ssem, rsem):
        return (
            remote(down_src, above_dst, ssem.at[0], rsem.at[0], {"slab": below_id}),
            remote(up_src, below_dst, ssem.at[1], rsem.at[1], {"slab": above_id}),
        )

    load_k.wait()
    kzup[...] = top_row(lambda j: kk[2, j])
    pl.semaphore_wait(barrier, n_s - 1 + len(OFFSETS))
    k_halo = halo(kk.at[2, 0], kzup, kza, kzb, ks, kr)
    for cpy in k_halo:
        cpy.start()
    load_f.wait()

    zero = jnp.zeros((height, width), jnp.float32)
    for buf in (z0, q1):
        for c in range(3):
            buf[c, 0] = zero
            buf[c, 9] = zero
    kz[8] = zero
    acc[...] = jnp.zeros_like(acc)

    def faces(k, carry):
        on = lane_on * (k < a).astype(jnp.float32)
        kx = kk[0, k] * on
        ky = kk[1, k] * on
        kz[k] = kk[2, k] * on
        x_up = pltpu.roll(kx, width - 1, 1)
        x_up = jnp.where(lane < width - 1, x_up, 0.0)
        x_down = jnp.where(lane > 0, pltpu.roll(kx, 1, 1), 0.0)
        gx[k] = jnp.where(lane < nx - 1, 0.5 * (kx + x_up), 0.0)
        y_up = jnp.where(row < height - 1, pltpu.roll(ky, height - 1, 0), 0.0)
        y_down = jnp.where(row > 0, pltpu.roll(ky, 1, 0), 0.0)
        gy[k] = jnp.where(row < height - 1, 0.5 * (ky + y_up), 0.0)
        sum_x = kx + 0.5 * (x_up + x_down)
        sum_y = ky + 0.5 * (y_up + y_down)
        for c in range(3):
            rj[c, k] = cp[c][c] + cf[c][0] * sum_x + cf[c][1] * sum_y
            f[c, k] = f[c, k] * on
        return carry

    lax.fori_loop(0, 8, faces, 0)

    for cpy in k_halo:
        cpy.wait()
    fz[0] = 0.5 * (kzb[...] * (lane_on * has_below) + kz[0])
    rim_k = kza[...] * (lane_on * has_above)

    def z_faces(j, carry):
        top = (j == a).astype(jnp.float32)
        fz[j] = 0.5 * (kz[j - 1] + kz[j] + top * rim_k)
        return carry

    lax.fori_loop(1, 9, z_faces, 0)

    def jacobi(c, k):
        return f[c, k] * (1.0 / (rj[c, k] + cf[c][2] * (fz[k] + fz[k + 1])))

    for c in range(3):
        z0[c, 1] = jacobi(c, 0)
        up[c] = jacobi(c, a - 1)
    z_halo = halo(z0.at[:, 1], up, za, zb, zs, zr)
    for cpy in z_halo:
        cpy.start()

    def invert(k):
        sum_z = fz[k] + fz[k + 1]
        for c in range(3):
            rj[c, k] = 1.0 / (rj[c, k] + cf[c][2] * sum_z)

    def first(k, carry):
        invert(k)
        for c in range(3):
            fc = f[c, k]
            zc = fc * rj[c, k]
            z0[c, k + 1] = zc
            acc[0] += fold8(fc * zc)
        return carry

    invert(0)
    for c in range(3):
        acc[0] += fold8(f[c, 0] * z0[c, 1])
    lax.fori_loop(1, 8, first, 0)

    def apply_row(u, base, c, k, values):
        uc = values[c]
        out = base
        for e in range(3):
            if e != c:
                out = out + cp[c][e] * values[e]
        gxk = gx[k]
        gyk = gy[k]
        nb_x = gxk * pltpu.roll(uc, width - 1, 1) + pltpu.roll(gxk * uc, 1, 1)
        nb_y = gyk * pltpu.roll(uc, height - 1, 0) + pltpu.roll(gyk * uc, 1, 0)
        inside = (k < a).astype(jnp.float32)
        nb_z = fz[k + 1] * u[c, k + 2] + (inside * fz[k]) * u[c, k]
        return out - (cf[c][0] * nb_x + cf[c][1] * nb_y + cf[c][2] * nb_z)

    def second(k, carry):
        values = [z0[c, k + 1] for c in range(3)]
        for c in range(3):
            w[c, k] = apply_row(z0, f[c, k], c, k, values)
        return carry

    lax.fori_loop(0, 8, second, 0)
    for cpy in z_halo:
        cpy.wait()
    for c in range(3):
        zb[c] = zb[c] * has_below
        wc = w[c, 0] - cf[c][2] * (fz[0] * zb[c])
        w[c, 0] = wc
        q1[c, 1] = wc * rj[c, 0]
    q_down = remote(q1.at[:, 1], qa, qs.at[0], qr.at[0], {"slab": below_id})
    q_down.start()
    for c in range(3):
        za[c] = za[c] * has_above
        for i, j in enumerate(ROWS_UP):
            w[c, j] -= (sel[i] * cf[c][2]) * (fz[j + 1] * za[c])

    def sums_of(c, k, qc):
        wc = w[c, k]
        acc[1] += fold8(z0[c, k + 1] * wc)
        acc[2] += fold8(wc * qc)

    def third(k, carry):
        for c in range(3):
            qc = w[c, k] * rj[c, k]
            q1[c, k + 1] = qc
            sums_of(c, k, qc)
        return carry

    for c in range(3):
        sums_of(c, 0, q1[c, 1])
    lax.fori_loop(1, 8, third, 0)
    for c in range(3):
        qup[c] = top_row(lambda j: q1[c, j + 1])

    full = (a == 8).astype(jnp.float32)

    def rows_of(i):
        return pl.ds(pl.multiple_of(i * chunk, chunk), chunk)

    def await_from(dst, ssem, rsem, c, o):
        dy, dx = OFFSETS[o]
        source = peer_of(g, N_Y - dy, dx)
        ref = dst(source, c)
        remote(ref, ref, ssem.at[o], rsem.at[o], {"grp": source}).wait_recv()
        return source

    def fourth(k, carry):
        values = [q1[c, k + 1] for c in range(3)]
        for c in range(3):
            acc[3] += fold8(values[c] * apply_row(q1, w[c, k], c, k, values))
        return carry

    lax.fori_loop(0, 8, fourth, 0)
    fz_top = top_row(lambda j: fz[j + 1]) * (2.0 * has_above)
    q_down.wait()
    for c in range(3):
        acc[3] -= cf[c][2] * fold8(qup[c] * (fz_top * qa[c]))

    for i in range(4):
        mom[i : i + 1] = jnp.sum(acc[i], axis=0, keepdims=True)
    mom[4:8] = jnp.zeros((4, width), jnp.float32)
    m_out = []
    for o in range(1, n_s):
        to = (s + o) % n_s
        m_out.append(remote(mom, momr.at[s], ms.at[o - 1], mr.at[o - 1], {"slab": to}))
    for cpy in m_out:
        cpy.start()
    q_up = remote(qup, qb, qs.at[1], qr.at[1], {"slab": above_id})
    q_up.start()
    momr[s] = mom[...]
    for o in range(1, n_s):
        source = (s + n_s - o) % n_s
        remote(
            momr.at[source], momr.at[source], ms.at[o - 1], mr.at[o - 1], {"slab": source}
        ).wait_recv()
    total = momr[0]
    for i in range(1, n_s):
        total = total + momr[i]
    sums = jnp.sum(total, axis=1, keepdims=True)
    rz0, m1, m2, m3 = (sums[i : i + 1] for i in range(4))
    step0 = rz0 / m1
    rz1 = step0 * step0 * m2 - rz0
    beta = rz1 / rz0
    bend = m1 - 2.0 * step0 * m2 + step0 * step0 * m3
    step1 = jnp.clip(rz1 / (bend - beta * rz1 / step0), 0.25, 1024.0)
    on_z = jnp.broadcast_to(step0 + step1 * (1.0 + beta), (height, width))
    on_q = jnp.broadcast_to(-step1 * step0, (height, width))

    p_out = []

    def spread(src, dst, ssem, rsem):
        for o, (dy, dx) in enumerate(OFFSETS):
            to = peer_of(g, dy, dx)
            cpy = remote(src(rows_of(to)), dst, ssem.at[o], rsem.at[o], {"grp": to})
            cpy.start()
            p_out.append(cpy)

    odd = s % 2
    is_odd = odd.astype(jnp.float32)
    is_even = 1.0 - is_odd
    for c in range(3):
        if c == 2:
            q_up.wait()
            for e in range(3):
                rim_below = on_z * zb[e] + on_q * (qb[e] * has_below)
                rim_above = on_z * za[e] + on_q * (qa[e] * has_above)
                rim[e] = is_even * rim_below + is_odd * rim_above
            spread(lambda rows: rim.at[:, rows], rims.at[g], rs, rr)
        solved = [on_z * z0[c, k + 1] + on_q * q1[c, k + 1] for k in range(8)]
        for r in range(4):
            pu[c, r] = solved[r] + full * pltpu.roll(solved[r + 4], width // 2, 1)
        spread(lambda rows: pu.at[c, :, rows], ru[c].at[g], ps.at[c], pr.at[c])
        for k in range(8):
            out[0, c, k] = solved[k]
        ru[c][g] = pu[c, :, rows_of(g)]
    rims[g] = rim[:, rows_of(g)]

    lanes = lax.broadcasted_iota(jnp.int32, (chunk, width), 1)
    half = lanes // 2
    beside = jnp.where(lanes % 2 == 1, half + 1, half + (width - 1)) % width
    low = (lanes < width // 2).astype(jnp.float32)

    def mix(t, c):
        lx, lz = levels[0, t], levels[1, t]
        nx_t, a_t = sizes(lx, lz)
        ids = [neigh[i, t] for i in range(3)]
        there = [(i >= 0).astype(jnp.float32) for i in ids]
        n0, n1, n2 = (jnp.maximum(i, 0) for i in ids)
        full_t = (a_t == 8).astype(jnp.float32) * there[0]
        short = (a_t == 4).astype(jnp.float32)
        on_x = (lanes < nx_t).astype(jnp.float32)

        def between(n):
            ends = rims[n, c]
            joint = inner[c][n]
            below = is_even * ends + is_odd * joint
            above = is_even * joint + is_odd * ends
            near = [ru[c][n, k] for k in range(4)]
            beyond = [below] + near + [above]
            beyond[3] = near[2] + short * above
            result = []
            for k in range(8):
                m = k // 2
                other = near[m - 1] if k % 2 == 0 and m > 0 else beyond[m + 2 * (k % 2)]
                result.append(0.75 * near[m] + 0.25 * other)
            return result

        across = between(n1)
        both = between(n2)
        for k in range(8):
            if k < 4:
                v = there[0] * ru[c][n0, k]
            else:
                v = full_t * pltpu.roll(ru[c][n0, k - 4], width // 2, 1)
            v = v * low - there[2] * both[k]
            x = 0.75 * jnp.take_along_axis(v, half, axis=1) + 0.25 * jnp.take_along_axis(
                v, beside, axis=1
            )
            x = x + there[1] * across[k]
            corr[t, c, k] = x * (on_x * (k < a_t).astype(jnp.float32))

    def finish(source, c, ref):
        rows = rows_of(source)
        for k in range(8):
            out[0, c, k, rows] = out[0, c, k, rows] - ref[source, c, k]

    c_out = []
    for c in range(3):
        for o in range(len(OFFSETS)):
            await_from(lambda i, j: ru[j].at[i], ps.at[c], pr.at[c], c, o)
        for p in range(N_GRP):
            run = sizes(levels[0, p], levels[1, p])[1]
            top = (run == 4).astype(jnp.float32)
            last = top * ru[c][p, 3] + (1.0 - top) * ru[c][p, 1]
            inner_out[c][p] = is_even * last + is_odd * ru[c][p, 0]
        swap = remote(inner_out[c], inner[c], ds.at[c], dr.at[c], {"slab": s + 1 - 2 * odd})
        swap.start()
        if c == 0:
            for o in range(len(OFFSETS)):
                await_from(lambda i, j: rims.at[i], rs, rr, c, o)
        swap.wait()
        for o, (dy, dx) in enumerate(OFFSETS):
            to = peer_of(g, dy, dx)
            mix(to, c)
            cpy = remote(corr.at[to, c], rc.at[g, c], cs.at[c, o], cr.at[c, o], {"grp": to})
            cpy.start()
            c_out.append(cpy)
        mix(g, c)
        finish(g, c, corr)
    for c in range(3):
        for o in range(len(OFFSETS)):
            finish(await_from(lambda i, j: rc.at[i, j], cs.at[c], cr.at[c], c, o), c, rc)
    for cpy in m_out + p_out + c_out:
        cpy.wait_send()


def solution(mesh):
    n_s = mesh.shape["slab"]

    def per_device(forcing, stiffness, anisotropy, coupling, levels, neighbours):
        _, _, depth, height, width = forcing.shape
        anisotropy = jnp.transpose(anisotropy, (1, 0, 2))
        coupling = jnp.transpose(coupling, (1, 0, 2))
        levels = levels.T
        neighbours = neighbours.T
        chunk = height // N_GRP
        plane = (height, width)
        f32 = jnp.float32
        dma = pltpu.SemaphoreType.DMA
        anyspec = pl.BlockSpec(memory_space=pl.ANY)
        vm = lambda *shape: pltpu.VMEM(shape, f32)
        others = len(OFFSETS)
        scratch = [
            pltpu.SMEM(anisotropy.shape, f32), pltpu.SMEM(coupling.shape, f32),
            pltpu.SMEM(levels.shape, jnp.int32), pltpu.SMEM(neighbours.shape, jnp.int32),
            vm(3, 8, *plane), vm(3, 8, *plane), vm(9, *plane), vm(8, *plane), vm(8, *plane),
            vm(9, *plane), vm(3, 8, *plane), vm(3, 10, *plane), vm(3, 8, *plane),
            vm(3, 10, *plane),
            vm(*plane), vm(*plane), vm(*plane),
            vm(3, *plane), vm(3, *plane), vm(3, *plane),
            vm(3, *plane), vm(3, *plane), vm(3, *plane),
            vm(3, 4, *plane), vm(3, *plane), vm(N_GRP, 3, chunk, width),
            *(vm(N_GRP, 4, chunk, width) for _ in range(3)),
            *(vm(N_GRP, chunk, width) for _ in range(6)),
            vm(N_GRP, 3, 8, chunk, width), vm(N_GRP, 3, 8, chunk, width),
            vm(4, 8, width), vm(8, width), vm(n_s, 8, width),
            dma((6,)),
            dma((2,)), dma((2,)), dma((2,)), dma((2,)), dma((2,)), dma((2,)),
            dma((n_s - 1,)), dma((n_s - 1,)),
            dma((3, others)), dma((3, others)), dma((others,)), dma((others,)), dma((3,)), dma((3,)),
            dma((3, others)), dma((3, others)),
        ]
        return pl.pallas_call(
            functools.partial(body, n_s),
            out_shape=pltpu.VMEM(forcing.shape, f32),
            in_specs=[anyspec] * 6,
            out_specs=pl.BlockSpec(memory_space=pltpu.VMEM),
            scratch_shapes=scratch,
            compiler_params=pltpu.CompilerParams(
                collective_id=0, has_side_effects=True, vmem_limit_bytes=56 * 1024 * 1024
            ),
        )(forcing, stiffness, anisotropy, coupling, levels, neighbours)

    wide = P("grp", None, "slab", None, None)
    small = P("grp", None, None)
    return jax.shard_map(
        per_device,
        mesh=mesh,
        in_specs=(wide, wide, small, small, P(), P()),
        out_specs=wide,
        check_vma=False,
    )
```

```python
import functools
import jax
import jax.numpy as jnp
from jax import lax
from jax.experimental import pallas as pl
from jax.experimental.pallas import tpu as pltpu
from jax.sharding import PartitionSpec as P

MESH = pl.DeviceIdType.MESH
N_GRP = 8
N_Y = 4
OFFSETS = ((1, 0), (3, 0), (0, 1), (2, 0), (1, 1), (3, 1), (2, 1))
ROWS_UP = (1, 3, 7)


def peer_of(g, dy, dx):
    y, x = g // 2, g % 2
    return ((y + dy) % N_Y) * 2 + (x + dx) % 2


def fold8(v):
    total = v[0:8]
    for i in range(1, v.shape[0] // 8):
        total = total + v[8 * i : 8 * i + 8]
    return total


def body(
    n_s, f_hbm, k_hbm, aniso_hbm, coup_hbm, levels_hbm, neigh_hbm, out,
    aniso, coup, levels, neigh,
    f, kk, kz, gx, gy, fz, rj, z0, w, q1, kzup, kza, kzb, up, za, zb, qup, qa, qb,
    pu, rim, rims, ru0, ru1, ru2, si0, si1, si2, ri0, ri1, ri2, corr, rc, acc, mom, momr,
    in_sem, ks, kr, zs, zr, qs, qr, ms, mr, ps, pr, rs, rr, ds, dr, cs, cr,
):
    g = lax.axis_index("grp")
    s = lax.axis_index("slab")
    height, width = f.shape[2], f.shape[3]
    chunk = height // N_GRP
    below_id = (s + n_s - 1) % n_s
    above_id = (s + 1) % n_s

    ru = (ru0, ru1, ru2)
    inner_out = (si0, si1, si2)
    inner = (ri0, ri1, ri2)

    barrier = pltpu.get_barrier_semaphore()
    for o in range(1, n_s):
        pl.semaphore_signal(barrier, inc=1, device_id={"slab": (s + o) % n_s}, device_id_type=MESH)
    for dy, dx in OFFSETS:
        pl.semaphore_signal(barrier, inc=1, device_id={"grp": peer_of(g, dy, dx)}, device_id_type=MESH)
    load_k = pltpu.make_async_copy(k_hbm.at[0], kk, in_sem.at[0])
    load_f = pltpu.make_async_copy(f_hbm.at[0], f, in_sem.at[1])
    smalls = [
        pltpu.make_async_copy(src, dst, in_sem.at[2 + i])
        for i, (src, dst) in enumerate(
            ((levels_hbm, levels), (aniso_hbm, aniso), (coup_hbm, coup), (neigh_hbm, neigh))
        )
    ]
    for cpy in smalls:
        cpy.start()
    load_k.start()
    load_f.start()
    for cpy in smalls:
        cpy.wait()

    def sizes(lx, lz):
        nx = jnp.where(lx == 2, width, jnp.where(lx == 1, width // 2, width // 4))
        a = jnp.where(lz == 2, 8, jnp.where(lz == 1, 4, 2))
        return nx, a

    nx, a = sizes(levels[0, g], levels[1, g])
    sx = nx.astype(jnp.float32) * (1.0 / height)
    sz = (a * n_s).astype(jnp.float32) * (1.0 / height)
    scale = (sx * sx, 1.0, sz * sz)
    cf = [[aniso[c, 0, d] * scale[d] for d in range(3)] for c in range(3)]
    cp = [[coup[c, 0, e] for e in range(3)] for c in range(3)]
    sel = [(a == j + 1).astype(jnp.float32) for j in ROWS_UP]
    has_below = (s > 0).astype(jnp.float32)
    has_above = (s < n_s - 1).astype(jnp.float32)

    lane = lax.broadcasted_iota(jnp.int32, (height, width), 1)
    row = lax.broadcasted_iota(jnp.int32, (height, width), 0)
    lane_on = (lane < nx).astype(jnp.float32)

    def top_row(read):
        return sel[0] * read(1) + sel[1] * read(3) + sel[2] * read(7)

    def remote(src, dst, ssem, rsem, device_id):
        return pltpu.make_async_remote_copy(
            src_ref=src, dst_ref=dst, send_sem=ssem, recv_sem=rsem,
            device_id=device_id, device_id_type=MESH,
        )

    def halo(down_src, up_src, above_dst, below_dst, ssem, rsem):
        return (
            remote(down_src, above_dst, ssem.at[0], rsem.at[0], {"slab": below_id}),
            remote(up_src, below_dst, ssem.at[1], rsem.at[1], {"slab": above_id}),
        )

    load_k.wait()
    kzup[...] = top_row(lambda j: kk[2, j])
    pl.semaphore_wait(barrier, n_s - 1 + len(OFFSETS))
    k_halo = halo(kk.at[2, 0], kzup, kza, kzb, ks, kr)
    for cpy in k_halo:
        cpy.start()
    load_f.wait()

    zero = jnp.zeros((height, width), jnp.float32)
    for buf in (z0, q1):
        for c in range(3):
            buf[c, 0] = zero
            buf[c, 9] = zero
    kz[8] = zero
    acc[...] = jnp.zeros_like(acc)

    def faces(k, carry):
        on = lane_on * (k < a).astype(jnp.float32)
        kx = kk[0, k] * on
        ky = kk[1, k] * on
        kz[k] = kk[2, k] * on
        x_up = pltpu.roll(kx, width - 1, 1)
        x_up = jnp.where(lane < width - 1, x_up, 0.0)
        x_down = jnp.where(lane > 0, pltpu.roll(kx, 1, 1), 0.0)
        gx[k] = jnp.where(lane < nx - 1, 0.5 * (kx + x_up), 0.0)
        y_up = jnp.where(row < height - 1, pltpu.roll(ky, height - 1, 0), 0.0)
        y_down = jnp.where(row > 0, pltpu.roll(ky, 1, 0), 0.0)
        gy[k] = jnp.where(row < height - 1, 0.5 * (ky + y_up), 0.0)
        sum_x = kx + 0.5 * (x_up + x_down)
        sum_y = ky + 0.5 * (y_up + y_down)
        for c in range(3):
            rj[c, k] = cp[c][c] + cf[c][0] * sum_x + cf[c][1] * sum_y
            f[c, k] = f[c, k] * on
        return carry

    lax.fori_loop(0, 8, faces, 0)

    for cpy in k_halo:
        cpy.wait()
    fz[0] = 0.5 * (kzb[...] * (lane_on * has_below) + kz[0])
    rim_k = kza[...] * (lane_on * has_above)

    def z_faces(j, carry):
        top = (j == a).astype(jnp.float32)
        fz[j] = 0.5 * (kz[j - 1] + kz[j] + top * rim_k)
        return carry

    lax.fori_loop(1, 9, z_faces, 0)

    def jacobi(c, k):
        return f[c, k] * (1.0 / (rj[c, k] + cf[c][2] * (fz[k] + fz[k + 1])))

    for c in range(3):
        z0[c, 1] = jacobi(c, 0)
        up[c] = jacobi(c, a - 1)
    z_halo = halo(z0.at[:, 1], up, za, zb, zs, zr)
    for cpy in z_halo:
        cpy.start()

    def invert(k):
        sum_z = fz[k] + fz[k + 1]
        for c in range(3):
            rj[c, k] = 1.0 / (rj[c, k] + cf[c][2] * sum_z)

    def first(k, carry):
        invert(k)
        for c in range(3):
            fc = f[c, k]
            zc = fc * rj[c, k]
            z0[c, k + 1] = zc
            acc[0] += fold8(fc * zc)
        return carry

    invert(0)
    for c in range(3):
        acc[0] += fold8(f[c, 0] * z0[c, 1])
    lax.fori_loop(1, 8, first, 0)

    def apply_row(u, base, c, k, values):
        uc = values[c]
        out = base
        for e in range(3):
            if e != c:
                out = out + cp[c][e] * values[e]
        gxk = gx[k]
        gyk = gy[k]
        nb_x = gxk * pltpu.roll(uc, width - 1, 1) + pltpu.roll(gxk * uc, 1, 1)
        nb_y = gyk * pltpu.roll(uc, height - 1, 0) + pltpu.roll(gyk * uc, 1, 0)
        inside = (k < a).astype(jnp.float32)
        nb_z = fz[k + 1] * u[c, k + 2] + (inside * fz[k]) * u[c, k]
        return out - (cf[c][0] * nb_x + cf[c][1] * nb_y + cf[c][2] * nb_z)

    def second(k, carry):
        values = [z0[c, k + 1] for c in range(3)]
        for c in range(3):
            w[c, k] = apply_row(z0, f[c, k], c, k, values)
        return carry

    lax.fori_loop(0, 8, second, 0)
    for cpy in z_halo:
        cpy.wait()
    for c in range(3):
        zb[c] = zb[c] * has_below
        wc = w[c, 0] - cf[c][2] * (fz[0] * zb[c])
        w[c, 0] = wc
        q1[c, 1] = wc * rj[c, 0]
    q_down = remote(q1.at[:, 1], qa, qs.at[0], qr.at[0], {"slab": below_id})
    q_down.start()
    for c in range(3):
        za[c] = za[c] * has_above
        for i, j in enumerate(ROWS_UP):
            w[c, j] -= (sel[i] * cf[c][2]) * (fz[j + 1] * za[c])

    def sums_of(c, k, qc):
        wc = w[c, k]
        acc[1] += fold8(z0[c, k + 1] * wc)
        acc[2] += fold8(wc * qc)

    def third(k, carry):
        for c in range(3):
            qc = w[c, k] * rj[c, k]
            q1[c, k + 1] = qc
            sums_of(c, k, qc)
        return carry

    for c in range(3):
        sums_of(c, 0, q1[c, 1])
    lax.fori_loop(1, 8, third, 0)
    for c in range(3):
        qup[c] = top_row(lambda j: q1[c, j + 1])

    full = (a == 8).astype(jnp.float32)

    def rows_of(i):
        return pl.ds(pl.multiple_of(i * chunk, chunk), chunk)

    def await_from(dst, ssem, rsem, c, o):
        dy, dx = OFFSETS[o]
        source = peer_of(g, N_Y - dy, dx)
        ref = dst(source, c)
        remote(ref, ref, ssem.at[o], rsem.at[o], {"grp": source}).wait_recv()
        return source

    def fourth(k, carry):
        values = [q1[c, k + 1] for c in range(3)]
        for c in range(3):
            acc[3] += fold8(values[c] * apply_row(q1, w[c, k], c, k, values))
        return carry

    lax.fori_loop(0, 8, fourth, 0)
    fz_top = top_row(lambda j: fz[j + 1]) * (2.0 * has_above)
    q_down.wait()
    for c in range(3):
        acc[3] -= cf[c][2] * fold8(qup[c] * (fz_top * qa[c]))

    for i in range(4):
        mom[i : i + 1] = jnp.sum(acc[i], axis=0, keepdims=True)
    m_out = []
    for o in range(1, n_s):
        to = (s + o) % n_s
        m_out.append(remote(mom, momr.at[s], ms.at[o - 1], mr.at[o - 1], {"slab": to}))
    for cpy in m_out:
        cpy.start()
    q_up = remote(qup, qb, qs.at[1], qr.at[1], {"slab": above_id})
    q_up.start()
    momr[s] = mom[...]
    for o in range(1, n_s):
        source = (s + n_s - o) % n_s
        remote(
            momr.at[source], momr.at[source], ms.at[o - 1], mr.at[o - 1], {"slab": source}
        ).wait_recv()
    total = momr[0]
    for i in range(1, n_s):
        total = total + momr[i]
    sums = jnp.sum(total, axis=1, keepdims=True)
    rz0, m1, m2, m3 = (sums[i : i + 1] for i in range(4))
    step0 = rz0 / m1
    rz1 = step0 * step0 * m2 - rz0
    beta = rz1 / rz0
    bend = m1 - 2.0 * step0 * m2 + step0 * step0 * m3
    step1 = jnp.clip(rz1 / (bend - beta * rz1 / step0), 0.25, 1024.0)
    on_z = jnp.broadcast_to(step0 + step1 * (1.0 + beta), (height, width))
    on_q = jnp.broadcast_to(-step1 * step0, (height, width))

    p_out = []

    def spread(src, dst, ssem, rsem):
        for o, (dy, dx) in enumerate(OFFSETS):
            to = peer_of(g, dy, dx)
            cpy = remote(src(rows_of(to)), dst, ssem.at[o], rsem.at[o], {"grp": to})
            cpy.start()
            p_out.append(cpy)

    odd = s % 2
    is_odd = odd.astype(jnp.float32)
    is_even = 1.0 - is_odd
    for c in range(3):
        if c == 2:
            q_up.wait()
            for e in range(3):
                rim_below = on_z * zb[e] + on_q * (qb[e] * has_below)
                rim_above = on_z * za[e] + on_q * (qa[e] * has_above)
                rim[e] = is_even * rim_below + is_odd * rim_above
            spread(lambda rows: rim.at[:, rows], rims.at[g], rs, rr)
        solved = [on_z * z0[c, k + 1] + on_q * q1[c, k + 1] for k in range(8)]
        for r in range(4):
            pu[c, r] = solved[r] + full * pltpu.roll(solved[r + 4], width // 2, 1)
        spread(lambda rows: pu.at[c, :, rows], ru[c].at[g], ps.at[c], pr.at[c])
        for k in range(8):
            out[0, c, k] = solved[k]
        ru[c][g] = pu[c, :, rows_of(g)]
    rims[g] = rim[:, rows_of(g)]

    lanes = lax.broadcasted_iota(jnp.int32, (chunk, width), 1)
    half = lanes // 2
    beside = jnp.where(lanes % 2 == 1, half + 1, half + (width - 1)) % width
    low = (lanes < width // 2).astype(jnp.float32)

    def mix(t, c):
        lx, lz = levels[0, t], levels[1, t]
        nx_t, a_t = sizes(lx, lz)
        ids = [neigh[i, t] for i in range(3)]
        there = [(i >= 0).astype(jnp.float32) for i in ids]
        n0, n1, n2 = (jnp.maximum(i, 0) for i in ids)
        full_t = (a_t == 8).astype(jnp.float32) * there[0]
        short = (a_t == 4).astype(jnp.float32)
        on_x = (lanes < nx_t).astype(jnp.float32)

        def between(n):
            ends = rims[n, c]
            joint = inner[c][n]
            below = is_even * ends + is_odd * joint
            above = is_even * joint + is_odd * ends
            near = [ru[c][n, k] for k in range(4)]
            beyond = [below] + near + [above]
            beyond[3] = near[2] + short * above
            result = []
            for k in range(8):
                m = k // 2
                other = near[m - 1] if k % 2 == 0 and m > 0 else beyond[m + 2 * (k % 2)]
                result.append(0.75 * near[m] + 0.25 * other)
            return result

        across = between(n1)
        both = between(n2)
        for k in range(8):
            if k < 4:
                v = there[0] * ru[c][n0, k]
            else:
                v = full_t * pltpu.roll(ru[c][n0, k - 4], width // 2, 1)
            v = v * low - there[2] * both[k]
            x = 0.75 * jnp.take_along_axis(v, half, axis=1) + 0.25 * jnp.take_along_axis(
                v, beside, axis=1
            )
            x = x + there[1] * across[k]
            corr[t, c, k] = x * (on_x * (k < a_t).astype(jnp.float32))

    def finish(source, c, ref):
        rows = rows_of(source)
        for k in range(8):
            out[0, c, k, rows] = out[0, c, k, rows] - ref[source, c, k]

    def answer_copy(c, o):
        to = peer_of(g, o // 2, o % 2)
        return remote(corr.at[to, c], rc.at[g, c], cs.at[c, o - 1], cr.at[c, o - 1], {"grp": to})

    def end_answer(o, carry):
        for c in range(3):
            answer_copy(c, o).wait_send()
        return carry

    for c in range(3):
        for o in range(len(OFFSETS)):
            await_from(lambda i, j: ru[j].at[i], ps.at[c], pr.at[c], c, o)
        for p in range(N_GRP):
            run = sizes(levels[0, p], levels[1, p])[1]
            top = (run == 4).astype(jnp.float32)
            last = top * ru[c][p, 3] + (1.0 - top) * ru[c][p, 1]
            inner_out[c][p] = is_even * last + is_odd * ru[c][p, 0]
        swap = remote(inner_out[c], inner[c], ds.at[c], dr.at[c], {"slab": s + 1 - 2 * odd})
        swap.start()
        if c == 0:
            for o in range(len(OFFSETS)):
                await_from(lambda i, j: rims.at[i], rs, rr, c, o)
        swap.wait()

        def answer(o, carry):
            to = peer_of(g, o // 2, o % 2)
            mix(to, c)
            answer_copy(c, o).start()
            return carry

        lax.fori_loop(1, N_GRP, answer, 0)
        mix(g, c)
        finish(g, c, corr)
    for c in range(3):
        for o in range(len(OFFSETS)):
            dy, dx = OFFSETS[o]
            source = peer_of(g, N_Y - dy, dx)
            ref = rc.at[source, c]
            i = 2 * dy + dx - 1
            remote(ref, ref, cs.at[c, i], cr.at[c, i], {"grp": source}).wait_recv()
            finish(source, c, rc)
    lax.fori_loop(1, N_GRP, end_answer, 0)
    for cpy in m_out + p_out:
        cpy.wait_send()


def solution(mesh):
    n_s = mesh.shape["slab"]

    def per_device(forcing, stiffness, anisotropy, coupling, levels, neighbours):
        _, _, depth, height, width = forcing.shape
        anisotropy = jnp.transpose(anisotropy, (1, 0, 2))
        coupling = jnp.transpose(coupling, (1, 0, 2))
        levels = levels.T
        neighbours = neighbours.T
        chunk = height // N_GRP
        plane = (height, width)
        f32 = jnp.float32
        dma = pltpu.SemaphoreType.DMA
        anyspec = pl.BlockSpec(memory_space=pl.ANY)
        vm = lambda *shape: pltpu.VMEM(shape, f32)
        others = len(OFFSETS)
        scratch = [
            pltpu.SMEM(anisotropy.shape, f32), pltpu.SMEM(coupling.shape, f32),
            pltpu.SMEM(levels.shape, jnp.int32), pltpu.SMEM(neighbours.shape, jnp.int32),
            vm(3, 8, *plane), vm(3, 8, *plane), vm(9, *plane), vm(8, *plane), vm(8, *plane),
            vm(9, *plane), vm(3, 8, *plane), vm(3, 10, *plane), vm(3, 8, *plane),
            vm(3, 10, *plane),
            vm(*plane), vm(*plane), vm(*plane),
            vm(3, *plane), vm(3, *plane), vm(3, *plane),
            vm(3, *plane), vm(3, *plane), vm(3, *plane),
            vm(3, 4, *plane), vm(3, *plane), vm(N_GRP, 3, chunk, width),
            *(vm(N_GRP, 4, chunk, width) for _ in range(3)),
            *(vm(N_GRP, chunk, width) for _ in range(6)),
            vm(N_GRP, 3, 8, chunk, width), vm(N_GRP, 3, 8, chunk, width),
            vm(4, 8, width), vm(4, width), vm(n_s, 4, width),
            dma((6,)),
            dma((2,)), dma((2,)), dma((2,)), dma((2,)), dma((2,)), dma((2,)),
            dma((n_s - 1,)), dma((n_s - 1,)),
            dma((3, others)), dma((3, others)), dma((others,)), dma((others,)), dma((3,)), dma((3,)),
            dma((3, others)), dma((3, others)),
        ]
        return pl.pallas_call(
            functools.partial(body, n_s),
            out_shape=pltpu.VMEM(forcing.shape, f32),
            in_specs=[anyspec] * 6,
            out_specs=pl.BlockSpec(memory_space=pltpu.VMEM),
            scratch_shapes=scratch,
            compiler_params=pltpu.CompilerParams(
                collective_id=0, has_side_effects=True, vmem_limit_bytes=56 * 1024 * 1024
            ),
        )(forcing, stiffness, anisotropy, coupling, levels, neighbours)

    wide = P("grp", None, "slab", None, None)
    small = P("grp", None, None)
    return jax.shard_map(
        per_device,
        mesh=mesh,
        in_specs=(wide, wide, small, small, P(), P()),
        out_specs=wide,
        check_vma=False,
    )
```

```python
import functools
import jax
import jax.numpy as jnp
from jax import lax
from jax.experimental import pallas as pl
from jax.experimental.pallas import tpu as pltpu
from jax.sharding import PartitionSpec as P

MESH = pl.DeviceIdType.MESH
N_GRP = 8
N_Y = 4
OFFSETS = ((1, 0), (3, 0), (0, 1), (2, 0), (1, 1), (3, 1), (2, 1))
ROWS_UP = (1, 3, 7)


def peer_of(g, dy, dx):
    y, x = g // 2, g % 2
    return ((y + dy) % N_Y) * 2 + (x + dx) % 2


def fold8(v):
    total = v[0:8]
    for i in range(1, v.shape[0] // 8):
        total = total + v[8 * i : 8 * i + 8]
    return total


def body(
    n_s, f_hbm, k_hbm, aniso_hbm, coup_hbm, levels_hbm, neigh_hbm, out,
    aniso, coup, levels, neigh,
    f, kk, kz, gx, gy, fz, rj, z0, w, q1, kzup, kza, kzb, up, za, zb, qup, qa, qb,
    pu, rim, rims, ru0, ru1, ru2, si0, si1, si2, ri0, ri1, ri2, corr, rc, acc, mom, momr,
    in_sem, ks, kr, zs, zr, qs, qr, ms, mr, ps, pr, rs, rr, ds, dr, cs, cr,
):
    g = lax.axis_index("grp")
    s = lax.axis_index("slab")
    height, width = f.shape[2], f.shape[3]
    chunk = height // N_GRP
    below_id = (s + n_s - 1) % n_s
    above_id = (s + 1) % n_s

    ru = (ru0, ru1, ru2)
    inner_out = (si0, si1, si2)
    inner = (ri0, ri1, ri2)

    barrier = pltpu.get_barrier_semaphore()
    for o in range(1, n_s):
        pl.semaphore_signal(barrier, inc=1, device_id={"slab": (s + o) % n_s}, device_id_type=MESH)
    for dy, dx in OFFSETS:
        pl.semaphore_signal(barrier, inc=1, device_id={"grp": peer_of(g, dy, dx)}, device_id_type=MESH)
    load_k = pltpu.make_async_copy(k_hbm.at[0], kk, in_sem.at[0])
    load_f = pltpu.make_async_copy(f_hbm.at[0], f, in_sem.at[1])
    smalls = [
        pltpu.make_async_copy(src, dst, in_sem.at[2 + i])
        for i, (src, dst) in enumerate(
            ((levels_hbm, levels), (aniso_hbm, aniso), (coup_hbm, coup), (neigh_hbm, neigh))
        )
    ]
    for cpy in smalls:
        cpy.start()
    load_k.start()
    load_f.start()
    for cpy in smalls:
        cpy.wait()

    def sizes(lx, lz):
        nx = jnp.where(lx == 2, width, jnp.where(lx == 1, width // 2, width // 4))
        a = jnp.where(lz == 2, 8, jnp.where(lz == 1, 4, 2))
        return nx, a

    nx, a = sizes(levels[0, g], levels[1, g])
    sx = nx.astype(jnp.float32) * (1.0 / height)
    sz = (a * n_s).astype(jnp.float32) * (1.0 / height)
    scale = (sx * sx, 1.0, sz * sz)
    cf = [[aniso[c, 0, d] * scale[d] for d in range(3)] for c in range(3)]
    cp = [[coup[c, 0, e] for e in range(3)] for c in range(3)]
    sel = [(a == j + 1).astype(jnp.float32) for j in ROWS_UP]
    has_below = (s > 0).astype(jnp.float32)
    has_above = (s < n_s - 1).astype(jnp.float32)

    lane = lax.broadcasted_iota(jnp.int32, (height, width), 1)
    row = lax.broadcasted_iota(jnp.int32, (height, width), 0)
    lane_on = (lane < nx).astype(jnp.float32)

    def top_row(read):
        return sel[0] * read(1) + sel[1] * read(3) + sel[2] * read(7)

    def remote(src, dst, ssem, rsem, device_id):
        return pltpu.make_async_remote_copy(
            src_ref=src, dst_ref=dst, send_sem=ssem, recv_sem=rsem,
            device_id=device_id, device_id_type=MESH,
        )

    def halo(down_src, up_src, above_dst, below_dst, ssem, rsem):
        return (
            remote(down_src, above_dst, ssem.at[0], rsem.at[0], {"slab": below_id}),
            remote(up_src, below_dst, ssem.at[1], rsem.at[1], {"slab": above_id}),
        )

    load_k.wait()
    kzup[...] = top_row(lambda j: kk[2, j])
    pl.semaphore_wait(barrier, n_s - 1 + len(OFFSETS))
    k_halo = halo(kk.at[2, 0], kzup, kza, kzb, ks, kr)
    for cpy in k_halo:
        cpy.start()
    load_f.wait()

    zero = jnp.zeros((height, width), jnp.float32)
    for buf in (z0, q1):
        for c in range(3):
            buf[c, 0] = zero
            buf[c, 9] = zero
    kz[8] = zero
    acc[...] = jnp.zeros_like(acc)

    def faces(k, carry):
        on = lane_on * (k < a).astype(jnp.float32)
        kx = kk[0, k] * on
        ky = kk[1, k] * on
        kz[k] = kk[2, k] * on
        x_up = pltpu.roll(kx, width - 1, 1)
        x_up = jnp.where(lane < width - 1, x_up, 0.0)
        x_down = jnp.where(lane > 0, pltpu.roll(kx, 1, 1), 0.0)
        gx[k] = jnp.where(lane < nx - 1, 0.5 * (kx + x_up), 0.0)
        y_up = jnp.where(row < height - 1, pltpu.roll(ky, height - 1, 0), 0.0)
        y_down = jnp.where(row > 0, pltpu.roll(ky, 1, 0), 0.0)
        gy[k] = jnp.where(row < height - 1, 0.5 * (ky + y_up), 0.0)
        sum_x = kx + 0.5 * (x_up + x_down)
        sum_y = ky + 0.5 * (y_up + y_down)
        for c in range(3):
            rj[c, k] = cp[c][c] + cf[c][0] * sum_x + cf[c][1] * sum_y
            f[c, k] = f[c, k] * on
        return carry

    lax.fori_loop(0, 8, faces, 0)

    for cpy in k_halo:
        cpy.wait()
    fz[0] = 0.5 * (kzb[...] * (lane_on * has_below) + kz[0])
    rim_k = kza[...] * (lane_on * has_above)

    def z_faces(j, carry):
        top = (j == a).astype(jnp.float32)
        fz[j] = 0.5 * (kz[j - 1] + kz[j] + top * rim_k)
        return carry

    lax.fori_loop(1, 9, z_faces, 0)

    def jacobi(c, k):
        return f[c, k] * (1.0 / (rj[c, k] + cf[c][2] * (fz[k] + fz[k + 1])))

    for c in range(3):
        z0[c, 1] = jacobi(c, 0)
        up[c] = jacobi(c, a - 1)
    z_halo = halo(z0.at[:, 1], up, za, zb, zs, zr)
    for cpy in z_halo:
        cpy.start()

    def invert(k):
        sum_z = fz[k] + fz[k + 1]
        for c in range(3):
            rj[c, k] = 1.0 / (rj[c, k] + cf[c][2] * sum_z)

    def first(k, carry):
        invert(k)
        for c in range(3):
            fc = f[c, k]
            zc = fc * rj[c, k]
            z0[c, k + 1] = zc
            acc[0] += fold8(fc * zc)
        return carry

    invert(0)
    for c in range(3):
        acc[0] += fold8(f[c, 0] * z0[c, 1])
    lax.fori_loop(1, 8, first, 0)

    def apply_row(u, base, c, k, values):
        uc = values[c]
        out = base
        for e in range(3):
            if e != c:
                out = out + cp[c][e] * values[e]
        gxk = gx[k]
        gyk = gy[k]
        nb_x = gxk * pltpu.roll(uc, width - 1, 1) + pltpu.roll(gxk * uc, 1, 1)
        nb_y = gyk * pltpu.roll(uc, height - 1, 0) + pltpu.roll(gyk * uc, 1, 0)
        inside = (k < a).astype(jnp.float32)
        nb_z = fz[k + 1] * u[c, k + 2] + (inside * fz[k]) * u[c, k]
        return out - (cf[c][0] * nb_x + cf[c][1] * nb_y + cf[c][2] * nb_z)

    def second(k, carry):
        values = [z0[c, k + 1] for c in range(3)]
        for c in range(3):
            w[c, k] = apply_row(z0, f[c, k], c, k, values)
        return carry

    lax.fori_loop(0, 8, second, 0)
    for cpy in z_halo:
        cpy.wait()
    for c in range(3):
        zb[c] = zb[c] * has_below
        wc = w[c, 0] - cf[c][2] * (fz[0] * zb[c])
        w[c, 0] = wc
        q1[c, 1] = wc * rj[c, 0]
    q_down = remote(q1.at[:, 1], qa, qs.at[0], qr.at[0], {"slab": below_id})
    q_down.start()
    for c in range(3):
        za[c] = za[c] * has_above
        for i, j in enumerate(ROWS_UP):
            w[c, j] -= (sel[i] * cf[c][2]) * (fz[j + 1] * za[c])

    def sums_of(c, k, qc):
        wc = w[c, k]
        acc[1] += fold8(z0[c, k + 1] * wc)
        acc[2] += fold8(wc * qc)

    def third(k, carry):
        for c in range(3):
            qc = w[c, k] * rj[c, k]
            q1[c, k + 1] = qc
            sums_of(c, k, qc)
        return carry

    for c in range(3):
        sums_of(c, 0, q1[c, 1])
    lax.fori_loop(1, 8, third, 0)
    for c in range(3):
        qup[c] = top_row(lambda j: q1[c, j + 1])

    full = (a == 8).astype(jnp.float32)

    def rows_of(i):
        return pl.ds(pl.multiple_of(i * chunk, chunk), chunk)

    def await_from(dst, ssem, rsem, c, o):
        dy, dx = OFFSETS[o]
        source = peer_of(g, N_Y - dy, dx)
        ref = dst(source, c)
        remote(ref, ref, ssem.at[o], rsem.at[o], {"grp": source}).wait_recv()
        return source

    def fourth(k, carry):
        values = [q1[c, k + 1] for c in range(3)]
        for c in range(3):
            acc[3] += fold8(values[c] * apply_row(q1, w[c, k], c, k, values))
        return carry

    lax.fori_loop(0, 8, fourth, 0)
    fz_top = top_row(lambda j: fz[j + 1]) * (2.0 * has_above)
    q_down.wait()
    for c in range(3):
        acc[3] -= cf[c][2] * fold8(qup[c] * (fz_top * qa[c]))

    for i in range(4):
        mom[i : i + 1] = jnp.sum(acc[i], axis=0, keepdims=True)
    m_out = []
    for o in range(1, n_s):
        to = (s + o) % n_s
        m_out.append(remote(mom, momr.at[s], ms.at[o - 1], mr.at[o - 1], {"slab": to}))
    for cpy in m_out:
        cpy.start()
    q_up = remote(qup, qb, qs.at[1], qr.at[1], {"slab": above_id})
    q_up.start()
    momr[s] = mom[...]
    for o in range(1, n_s):
        source = (s + n_s - o) % n_s
        remote(
            momr.at[source], momr.at[source], ms.at[o - 1], mr.at[o - 1], {"slab": source}
        ).wait_recv()
    total = momr[0]
    for i in range(1, n_s):
        total = total + momr[i]
    sums = jnp.sum(total, axis=1, keepdims=True)
    rz0, m1, m2, m3 = (sums[i : i + 1] for i in range(4))
    step0 = rz0 / m1
    rz1 = step0 * step0 * m2 - rz0
    beta = rz1 / rz0
    bend = m1 - 2.0 * step0 * m2 + step0 * step0 * m3
    step1 = jnp.clip(rz1 / (bend - beta * rz1 / step0), 0.25, 1024.0)
    on_z = jnp.broadcast_to(step0 + step1 * (1.0 + beta), (height, width))
    on_q = jnp.broadcast_to(-step1 * step0, (height, width))

    p_out = []

    def spread(src, dst, ssem, rsem):
        for o, (dy, dx) in enumerate(OFFSETS):
            to = peer_of(g, dy, dx)
            cpy = remote(src(rows_of(to)), dst, ssem.at[o], rsem.at[o], {"grp": to})
            cpy.start()
            p_out.append(cpy)

    odd = s % 2
    is_odd = odd.astype(jnp.float32)
    is_even = 1.0 - is_odd
    for c in range(3):
        if c == 2:
            q_up.wait()
            for e in range(3):
                rim_below = on_z * zb[e] + on_q * (qb[e] * has_below)
                rim_above = on_z * za[e] + on_q * (qa[e] * has_above)
                rim[e] = is_even * rim_below + is_odd * rim_above
            spread(lambda rows: rim.at[:, rows], rims.at[g], rs, rr)
        solved = [on_z * z0[c, k + 1] + on_q * q1[c, k + 1] for k in range(8)]
        for r in range(4):
            pu[c, r] = solved[r] + full * pltpu.roll(solved[r + 4], width // 2, 1)
        spread(lambda rows: pu.at[c, :, rows], ru[c].at[g], ps.at[c], pr.at[c])
        for k in range(8):
            out[0, c, k] = solved[k]
        ru[c][g] = pu[c, :, rows_of(g)]
    rims[g] = rim[:, rows_of(g)]

    lanes = lax.broadcasted_iota(jnp.int32, (chunk, width), 1)
    half = lanes // 2
    beside = jnp.where(lanes % 2 == 1, half + 1, half + (width - 1)) % width
    low = (lanes < width // 2).astype(jnp.float32)

    def mix(t, c):
        lx, lz = levels[0, t], levels[1, t]
        nx_t, a_t = sizes(lx, lz)
        ids = [neigh[i, t] for i in range(3)]
        there = [(i >= 0).astype(jnp.float32) for i in ids]
        n0, n1, n2 = (jnp.maximum(i, 0) for i in ids)
        full_t = (a_t == 8).astype(jnp.float32) * there[0]
        short = (a_t == 4).astype(jnp.float32)
        on_x = (lanes < nx_t).astype(jnp.float32)

        def between(n):
            ends = rims[n, c]
            joint = inner[c][n]
            below = is_even * ends + is_odd * joint
            above = is_even * joint + is_odd * ends
            near = [ru[c][n, k] for k in range(4)]
            beyond = [below] + near + [above]
            beyond[3] = near[2] + short * above
            result = []
            for k in range(8):
                m = k // 2
                other = near[m - 1] if k % 2 == 0 and m > 0 else beyond[m + 2 * (k % 2)]
                result.append(0.75 * near[m] + 0.25 * other)
            return result

        across = between(n1)
        both = between(n2)
        for k in range(8):
            if k < 4:
                v = there[0] * ru[c][n0, k]
            else:
                v = full_t * pltpu.roll(ru[c][n0, k - 4], width // 2, 1)
            v = v * low - there[2] * both[k]
            x = 0.75 * jnp.take_along_axis(v, half, axis=1) + 0.25 * jnp.take_along_axis(
                v, beside, axis=1
            )
            x = x + there[1] * across[k]
            corr[t, c, k] = x * (on_x * (k < a_t).astype(jnp.float32))

    def finish(source, c, ref):
        rows = rows_of(source)
        for k in range(8):
            out[0, c, k, rows] = out[0, c, k, rows] - ref[source, c, k]

    def answer_copy(c, o):
        to = peer_of(g, o // 2, o % 2)
        return remote(corr.at[to, c], rc.at[g, c], cs.at[c, o - 1], cr.at[c, o - 1], {"grp": to})

    def end_answer(o, carry):
        for c in range(3):
            answer_copy(c, o).wait_send()
        return carry

    for c in range(3):
        for o in range(len(OFFSETS)):
            await_from(lambda i, j: ru[j].at[i], ps.at[c], pr.at[c], c, o)
        for p in range(N_GRP):
            run = sizes(levels[0, p], levels[1, p])[1]
            top = (run == 4).astype(jnp.float32)
            last = top * ru[c][p, 3] + (1.0 - top) * ru[c][p, 1]
            inner_out[c][p] = is_even * last + is_odd * ru[c][p, 0]
        swap = remote(inner_out[c], inner[c], ds.at[c], dr.at[c], {"slab": s + 1 - 2 * odd})
        swap.start()
        if c == 0:
            for o in range(len(OFFSETS)):
                await_from(lambda i, j: rims.at[i], rs, rr, c, o)
        swap.wait()

        def answer(i, carry):
            o = 1 + (i * (3 + 2 * odd) + 6) % 7
            to = peer_of(g, o // 2, o % 2)
            mix(to, c)
            answer_copy(c, o).start()
            return carry

        lax.fori_loop(1, N_GRP, answer, 0)
        mix(g, c)
        finish(g, c, corr)
    for c in range(3):
        for o in range(len(OFFSETS)):
            dy, dx = OFFSETS[o]
            source = peer_of(g, N_Y - dy, dx)
            ref = rc.at[source, c]
            i = 2 * dy + dx - 1
            remote(ref, ref, cs.at[c, i], cr.at[c, i], {"grp": source}).wait_recv()
            finish(source, c, rc)
    lax.fori_loop(1, N_GRP, end_answer, 0)
    for cpy in m_out + p_out:
        cpy.wait_send()


def solution(mesh):
    n_s = mesh.shape["slab"]

    def per_device(forcing, stiffness, anisotropy, coupling, levels, neighbours):
        _, _, depth, height, width = forcing.shape
        anisotropy = jnp.transpose(anisotropy, (1, 0, 2))
        coupling = jnp.transpose(coupling, (1, 0, 2))
        levels = levels.T
        neighbours = neighbours.T
        chunk = height // N_GRP
        plane = (height, width)
        f32 = jnp.float32
        dma = pltpu.SemaphoreType.DMA
        anyspec = pl.BlockSpec(memory_space=pl.ANY)
        vm = lambda *shape: pltpu.VMEM(shape, f32)
        others = len(OFFSETS)
        scratch = [
            pltpu.SMEM(anisotropy.shape, f32), pltpu.SMEM(coupling.shape, f32),
            pltpu.SMEM(levels.shape, jnp.int32), pltpu.SMEM(neighbours.shape, jnp.int32),
            vm(3, 8, *plane), vm(3, 8, *plane), vm(9, *plane), vm(8, *plane), vm(8, *plane),
            vm(9, *plane), vm(3, 8, *plane), vm(3, 10, *plane), vm(3, 8, *plane),
            vm(3, 10, *plane),
            vm(*plane), vm(*plane), vm(*plane),
            vm(3, *plane), vm(3, *plane), vm(3, *plane),
            vm(3, *plane), vm(3, *plane), vm(3, *plane),
            vm(3, 4, *plane), vm(3, *plane), vm(N_GRP, 3, chunk, width),
            *(vm(N_GRP, 4, chunk, width) for _ in range(3)),
            *(vm(N_GRP, chunk, width) for _ in range(6)),
            vm(N_GRP, 3, 8, chunk, width), vm(N_GRP, 3, 8, chunk, width),
            vm(4, 8, width), vm(4, width), vm(n_s, 4, width),
            dma((6,)),
            dma((2,)), dma((2,)), dma((2,)), dma((2,)), dma((2,)), dma((2,)),
            dma((n_s - 1,)), dma((n_s - 1,)),
            dma((3, others)), dma((3, others)), dma((others,)), dma((others,)), dma((3,)), dma((3,)),
            dma((3, others)), dma((3, others)),
        ]
        return pl.pallas_call(
            functools.partial(body, n_s),
            out_shape=pltpu.VMEM(forcing.shape, f32),
            in_specs=[anyspec] * 6,
            out_specs=pl.BlockSpec(memory_space=pltpu.VMEM),
            scratch_shapes=scratch,
            compiler_params=pltpu.CompilerParams(
                collective_id=0, has_side_effects=True, vmem_limit_bytes=56 * 1024 * 1024
            ),
        )(forcing, stiffness, anisotropy, coupling, levels, neighbours)

    wide = P("grp", None, "slab", None, None)
    small = P("grp", None, None)
    return jax.shard_map(
        per_device,
        mesh=mesh,
        in_specs=(wide, wide, small, small, P(), P()),
        out_specs=wide,
        check_vma=False,
    )
```
